512 devices in a mesh: blk: 32 (over z, y_lo), head: 16 (over x, y_hi, core).
Axes of the slice: x: 4, y: 8 (y_hi: 2, y_lo: 4; y = y_hi * 4 + y_lo), z: 8, core: 2. Of those that a mesh axis runs over, the one named last changes fastest.
Arguments:
- queries: bfloat16 [16384, 1024], P('blk', 'head'), may hold values from -170 to 170
- key_rows: bfloat16 [16384, 1024], P('blk', 'head'), may hold values from -9 to 9
- values: bfloat16 [16384, 1024], P('blk', 'head'), may hold values from -48 to 48
- text_keys: bfloat16 [1232, 1024], P(None, 'head'), may hold values from -9 to 9
- text_values: bfloat16 [1232, 1024], P(None, 'head'), may hold values from -48 to 48
- block_image: int32 [128], replicated, may hold values from 0 to 7, as said below
- gate_image: float32 [8, 1536], replicated, may hold values from 0.5 to 2
- residual: bfloat16 [16384, 1536], P(('blk', 'head')), may hold values from -6 to 6
- w_out: bfloat16 [1024, 1536], P('head'), may hold values from -0.1875 to 0.1875
Outputs:
- stream_out: bfloat16 [16384, 1536], P(('blk', 'head'))
The draws below stay inside these ranges and needn't reach their ends.
Inputs may be any that keep to these rules, and one draw needn't show every extreme that they name: `block_image`: each image number 0 to 7 names 8 to 24 of the entries, some image exactly 24 and some exactly 8; the blocks of an image lie anywhere in the array.
All inputs are finite; a program needn't handle non-finite values.
Results may differ from the reference program's by a relative error of at most 0.014.
Values may be sent and summed in bfloat16 or wider, within the bound.
A program may use at most 64 MiB of HBM per device.

```python
import math
import jax
import jax.numpy as jnp
from jax import lax

D = 1536
HEADS = 16
HD = 64
TEXT = 154
BS = 128
TOK_BLK = 512
NBLOCKS = 128
IMAGES = 8
TOKENS = 16384


def shared_keys(key):
    base = 1.5 * jax.random.normal(jax.random.fold_in(key, 7), (TOKENS, HEADS * HD), jnp.float32)
    base = jnp.clip(base, -9.0, 9.0)
    return base


def draw_key_rows(key, part):
    base = shared_keys(key)
    return base.astype(jnp.bfloat16)


def draw_queries(key, part):
    fresh = 1.5 * jax.random.normal(jax.random.fold_in(key, 9), (TOKENS, HEADS * HD), jnp.float32)
    fresh = jnp.clip(fresh, -9.0, 9.0)
    return fresh.astype(jnp.bfloat16)


def draw_block_image(key, part):
    pairs = IMAGES // 2
    split = jax.random.randint(jax.random.fold_in(key, 1), (pairs,), 8, 25)
    split = split.at[0].set(24)
    counts = jnp.stack([split, 32 - split], axis=1).reshape(IMAGES)
    labels = jax.random.permutation(jax.random.fold_in(key, 2), IMAGES).astype(jnp.int32)
    bounds = jnp.cumsum(counts)
    blocks = jnp.arange(NBLOCKS)
    sorted_slot = jnp.sum((blocks[:, None] >= bounds[None, :]).astype(jnp.int32), axis=1)
    image = labels[sorted_slot]
    order = jax.random.permutation(jax.random.fold_in(key, 3), NBLOCKS)
    return image[order].astype(jnp.int32)


def shard_levels(key, extent, shards, smallest, high):
    loudness = 1.0
    for position, blocks in shards:
        steps = jax.random.uniform(jax.random.fold_in(jax.random.fold_in(key, 6), position), (blocks,), jnp.float32, smallest / len(shards), high / len(shards))
        loudness = loudness * jnp.repeat(jnp.exp(steps), extent[position] // blocks).reshape((-1,) + (1,) * (len(extent) - 1 - position))
    return loudness


def centred(rng, extent, spread, reach, cuts=(), kind=jnp.bfloat16):
    values = spread * jax.random.normal(rng, extent, jnp.float32)
    if cuts:
        values = values * shard_levels(rng, extent, cuts, -0.22, 0.18)
    return jnp.clip(values, -reach, reach).astype(kind)


def setup_inputs(seed: int = 0) -> dict:
    splits = jax.random.split(jax.random.key(seed), 10)
    queries = draw_queries(jax.random.fold_in(splits[9], 71), 0)
    key_rows = draw_key_rows(jax.random.fold_in(splits[9], 71), 0)
    values = centred(splits[2], (TOKENS, HEADS * HD), 8.0, 48.0, ((0, 32), (1, 16)))
    text_keys = centred(splits[3], (IMAGES * TEXT, HEADS * HD), 1.5, 9.0, ((1, 16),))
    text_values = centred(splits[4], (IMAGES * TEXT, HEADS * HD), 8.0, 48.0, ((1, 16),))
    block_image = draw_block_image(jax.random.fold_in(splits[9], 71), 0)
    gate_image = jnp.clip(jax.random.uniform(splits[6], (IMAGES, D), jnp.float32, 0.5, 2.0), 0.5, 2.0)
    residual = centred(splits[7], (TOKENS, D), 1.0, 6.0, ((0, 512),))
    w_out = centred(splits[8], (HEADS * HD, D), (HEADS * HD) ** -0.5, 0.1875, ((0, 16),))
    return dict(queries=queries, key_rows=key_rows, values=values, text_keys=text_keys, text_values=text_values, block_image=block_image, gate_image=gate_image, residual=residual, w_out=w_out)


def reference(queries, key_rows, values, text_keys, text_values, block_image, gate_image, residual, w_out):
    token_image = jnp.repeat(block_image, BS).astype(jnp.int32)
    text_image = (jnp.arange(IMAGES * TEXT) // TEXT).astype(jnp.int32)
    every_key = jnp.concatenate([key_rows, text_keys], axis=0)
    every_value = jnp.concatenate([values, text_values], axis=0)
    key_image = jnp.concatenate([token_image, text_image], axis=0)
    scale = 1.0 / math.sqrt(HD)
    nkeys = every_key.shape[0]
    query_heads = queries.reshape(TOKENS, HEADS, HD).transpose(1, 0, 2)
    key_heads = every_key.reshape(nkeys, HEADS, HD).transpose(1, 0, 2)
    value_heads = every_value.reshape(nkeys, HEADS, HD).transpose(1, 0, 2)
    query_blocks = query_heads.reshape(HEADS, TOKENS // TOK_BLK, TOK_BLK, HD)
    image_blocks = token_image.reshape(TOKENS // TOK_BLK, TOK_BLK)

    def one_head(operands):
        qhead, khead, vhead = operands

        def one_block(inner):
            qblock, qimage = inner
            scores = jnp.dot(qblock, khead.T, preferred_element_type=jnp.float32) * scale
            allowed = qimage[:, None] == key_image[None, :]
            scores = jnp.where(allowed, scores, -1e+30)
            peak = lax.optimization_barrier(jnp.max(scores, axis=1, keepdims=True))
            expo = jnp.exp(scores - peak)
            denom = lax.optimization_barrier(jnp.sum(expo, axis=1, keepdims=True))
            numer = jnp.dot(expo.astype(jnp.bfloat16), vhead, preferred_element_type=jnp.float32)
            return (numer / denom).astype(jnp.bfloat16)
        return lax.map(one_block, (qhead, image_blocks))
    attended = lax.map(one_head, (query_blocks, key_heads, value_heads))
    attended = attended.reshape(HEADS, TOKENS, HD).transpose(1, 0, 2).reshape(TOKENS, HEADS * HD)
    projected = jnp.dot(attended, w_out, preferred_element_type=jnp.float32)
    gating = gate_image[token_image]
    return (residual.astype(jnp.float32) + gating * projected).astype(jnp.bfloat16)
```

```python
import functools
import math

import jax
import jax.numpy as jnp
from jax import lax
from jax.experimental import pallas as pl
from jax.experimental.pallas import tpu as pltpu
from jax.sharding import PartitionSpec as P

HD = 64
TEXT = 154
BS = 128
TOK = 512
YL = 4
ZL = 8
NH = 16
D = 1536
ROWS = TOK // NH
TSLOTS = 3
FAR = -(2.0**100)
RATE = math.log2(math.e) / math.sqrt(HD)
MESH = pl.DeviceIdType.MESH
BF = jnp.bfloat16
F32 = jnp.float32
NT = (((1,), (1,)), ((), ()))


def flip(index, mask, bits):
    total = 0
    for b in range(bits):
        bit = (index // (1 << b)) % 2
        total = total + (1 << b) * ((1 - bit) if (mask >> b) & 1 else bit)
    return total


def iota(shape, dim):
    return lax.broadcasted_iota(jnp.int32, shape, dim)


def kernel(
    q_ref, k_ref, v_ref, tk_ref, tv_ref, img_ref, gate_ref, res_ref, w_ref,
    out_ref,
    kv, qt, qa, ka, va, acc, mx, tpad, osend, orecv, ssend, srecv, attl, atth, arecv, wbuf,
    q_s, q_r, kv_s, kv_r, w_s, w_r, o_s, o_r, st_s, st_r, a_s, a_r,
):
    blk = lax.axis_index("blk")
    head = lax.axis_index("head")
    z = blk // YL
    y = blk % YL
    zright = ((z + 1) % ZL) * YL + y
    zleft = ((z + ZL - 1) % ZL) * YL + y
    ypeer = [z * YL + flip(y, c, 2) for c in range(YL)]
    hpeer = [flip(head, s, 4) for s in range(NH)]

    barrier = pltpu.get_barrier_semaphore()
    for other in (zright, zleft, ypeer[1], ypeer[2], ypeer[3]):
        pl.semaphore_signal(barrier, inc=1, device_id={"blk": other}, device_id_type=MESH)
    for s in range(1, NH):
        pl.semaphore_signal(barrier, inc=1, device_id={"head": hpeer[s]}, device_id_type=MESH)

    eye = (iota((HD, HD), 0) == iota((HD, HD), 1)).astype(F32).astype(BF)
    low = (iota((HD, 128), 0) == iota((HD, 128), 1)).astype(F32).astype(BF)
    high = (iota((HD, 128), 0) + HD == iota((HD, 128), 1)).astype(F32).astype(BF)

    pack = jnp.dot(k_ref[...], low, preferred_element_type=F32)
    pack = pack + jnp.dot(v_ref[...], high, preferred_element_type=F32)
    kv[0] = pack.astype(BF)
    qt[0] = lax.dot_general(eye, q_ref[...], NT, preferred_element_type=F32).astype(BF)

    pl.semaphore_wait(barrier, 5 + NH - 1)

    started = []

    def send(src, dst, ssem, rsem, dev):
        copy = pltpu.make_async_remote_copy(
            src_ref=src, dst_ref=dst, send_sem=ssem, recv_sem=rsem,
            device_id=dev, device_id_type=MESH,
        )
        copy.start()
        started.append(copy)
        return copy

    def q_copy(c):
        return send(qt.at[0], qt.at[c], q_s.at[c - 1], q_r.at[c - 1], {"blk": ypeer[c]})

    def kv_right(step):
        src = 0 if step == 1 else ZL - (step - 1)
        dst = ZL - step
        rows = pl.ds(0, TOK // 2) if step == 4 else pl.ds(0, TOK)
        return send(kv.at[src, rows], kv.at[dst, rows], kv_s.at[step - 1], kv_r.at[step - 1], {"blk": zright})

    def kv_left(step):
        rows = pl.ds(TOK // 2, TOK // 2) if step == 4 else pl.ds(0, TOK)
        return send(kv.at[step - 1, rows], kv.at[step, rows], kv_s.at[step + 3], kv_r.at[step + 3], {"blk": zleft})

    w_count = [0]

    def w_copy(origin, to):
        src = w_ref if origin == 0 else wbuf.at[pl.ds(origin * HD, HD)]
        slot = origin ^ to
        k = w_count[0]
        w_count[0] += 1
        return send(src, wbuf.at[pl.ds(slot * HD, HD)], w_s.at[k], w_r.at[slot], {"head": hpeer[to]})

    def w_wait(slot):
        part = wbuf.at[pl.ds(slot * HD, HD)]
        pltpu.make_async_remote_copy(
            src_ref=part, dst_ref=part, send_sem=w_s.at[0], recv_sem=w_r.at[slot],
            device_id={"head": hpeer[1]}, device_id_type=MESH,
        ).wait_recv()

    q_cps = [None] + [q_copy(c) for c in (1, 2, 3)]
    r_cps = {1: kv_right(1)}
    l_cps = {1: kv_left(1)}
    w_copy(0, 2)
    for s in (4, 12, 8):
        w_copy(0, s)
    w_copy(0, 1)
    wbuf[pl.ds(0, HD)] = w_ref[...]

    lane = iota((BS, 128), 1)

    def fill_keys(slot, packet, first_block):
        packf = packet.astype(F32)
        for b in range(TOK // BS):
            image = img_ref[first_block + b]
            gap = jnp.where((lane < HD + 8) & (lane != HD + image), FAR, 0.0)
            rows = jnp.where(lane < HD, packf[b * BS : (b + 1) * BS], gap)
            ka[slot, b * BS : (b + 1) * BS] = rows.astype(BF)
        vt = lax.dot_general(high, packet, NT, preferred_element_type=F32)
        va[slot, 0:HD] = vt.astype(BF)
        va[slot, HD : HD + 16] = jnp.ones((16, TOK), BF)

    def fill_queries(c):
        qa[c, 0:HD] = qt[c]
        first = ypeer[c] * (TOK // BS)
        for b in range(TOK // BS):
            image = img_ref[first + b]
            hot = (iota((16, BS), 0) == image).astype(F32)
            qa[c, HD : HD + 16, b * BS : (b + 1) * BS] = hot.astype(BF)
        qa[c, HD + 16 : 128] = jnp.zeros((128 - HD - 16, TOK), BF)

    def process(slot, c):
        keys = ka[slot]
        vals = va[slot]
        for part in range(2):
            cols = slice(part * 256, part * 256 + 256)
            sc = jnp.dot(keys, qa[c, :, cols], preferred_element_type=F32)
            old = mx[c, 0:1, cols]
            new = jnp.maximum(old, jnp.max(sc, axis=0, keepdims=True))
            pr = jnp.exp2((sc - new) * RATE).astype(BF)
            shrink = jnp.exp2((old - new) * RATE)
            upd = jnp.dot(vals, pr, preferred_element_type=F32)
            acc[c, :, cols] = acc[c, :, cols] * shrink + upd
            mx[c, 0:1, cols] = new

    for c in range(YL):
        acc[c] = jnp.zeros((HD + 16, TOK), F32)
        mx[c] = jnp.full((8, TOK), FAR, F32)

    fill_queries(0)
    ntext = tk_ref.shape[0]
    tpad[0, 0:ntext] = tk_ref[...]
    tpad[0, ntext:] = jnp.zeros((TSLOTS * TOK - ntext, HD), BF)
    tpad[1, 0:ntext] = tv_ref[...]
    tpad[1, ntext:] = jnp.zeros((TSLOTS * TOK - ntext, HD), BF)
    for t in range(TSLOTS):
        rows = iota((TOK, 128), 0) + t * TOK
        cols = iota((TOK, 128), 1) - HD
        inside = (rows >= cols * TEXT) & (rows < (cols + 1) * TEXT)
        gap = jnp.where((cols >= 0) & (cols < 8) & jnp.logical_not(inside), FAR, 0.0)
        tk = tpad[0, t * TOK : (t + 1) * TOK]
        tv = tpad[1, t * TOK : (t + 1) * TOK]
        ka[ZL + t] = (jnp.dot(tk, low, preferred_element_type=F32) + gap).astype(BF)
        va[ZL + t, 0:HD] = lax.dot_general(eye, tv, NT, preferred_element_type=F32).astype(BF)
        va[ZL + t, HD : HD + 16] = jnp.ones((16, TOK), BF)

    fill_keys(0, kv[0], blk * (TOK // BS))

    def own_step(t, carry):
        slot = (ZL + t) % (ZL + TSLOTS)
        process(slot, 0)
        return carry

    lax.fori_loop(0, TSLOTS + 1, own_step, 0)

    for c in (1, 2, 3):
        q_cps[c].wait_recv()
        fill_queries(c)

    def first_step(c, carry):
        process(0, c)
        return carry

    lax.fori_loop(1, YL, first_step, 0)

    def origin_block(slot):
        return (((z + slot) % ZL) * YL + y) * (TOK // BS)

    for step in (1, 2, 3):
        r_cps[step].wait_recv()
        r_cps[step + 1] = kv_right(step + 1)
        l_cps[step].wait_recv()
        l_cps[step + 1] = kv_left(step + 1)
        fill_keys(ZL - step, kv[ZL - step], origin_block(ZL - step))
        fill_keys(step, kv[step], origin_block(step))

        def mid_step(t, carry, step=step):
            side = t // YL
            slot = step + side * (ZL - 2 * step)
            process(slot, t % YL)
            return carry

        lax.fori_loop(0, 2 * YL, mid_step, 0)
        if step == 1:
            for s in (4, 12, 8):
                w_wait(s)
                w_copy(s, 1)
        if step == 2:
            w_wait(2)
            for s in (4, 12, 8):
                w_copy(2, s)
            w_copy(2, 1)

    r_cps[4].wait_recv()
    l_cps[4].wait_recv()
    fill_keys(4, kv[4], origin_block(4))
    o_cps = [None] * YL
    st_cps = [None] * YL
    for c in (3, 2, 1):
        process(4, c)
        osend[c - 1] = acc[c, 0:HD].astype(BF)
        ssend[c - 1, 0:1] = mx[c, 0:1]
        ssend[c - 1, 1:2] = acc[c, HD : HD + 1]
        ssend[c - 1, 2:8] = jnp.zeros((6, TOK), F32)
        dev = {"blk": ypeer[c]}
        o_cps[c] = send(osend.at[c - 1], orecv.at[c - 1], o_s.at[c - 1], o_r.at[c - 1], dev)
        st_cps[c] = send(ssend.at[c - 1], srecv.at[c - 1], st_s.at[c - 1], st_r.at[c - 1], dev)
    process(4, 0)
    for s in (6, 14, 10):
        w_wait(s)
        w_copy(s, 1)
    for c in (1, 2, 3):
        o_cps[c].wait_recv()
        st_cps[c].wait_recv()

    maxes = [mx[0, 0:1]] + [srecv[c - 1, 0:1] for c in (1, 2, 3)]
    sums = [acc[0, HD : HD + 1]] + [srecv[c - 1, 1:2] for c in (1, 2, 3)]
    top = functools.reduce(jnp.maximum, maxes)
    scales = [jnp.exp2((m - top) * RATE) for m in maxes]
    denom = functools.reduce(jnp.add, [s * l for s, l in zip(scales, sums)])
    numer = acc[0, 0:HD] * scales[0]
    for c in (1, 2, 3):
        numer = numer + orecv[c - 1].astype(F32) * scales[c]
    att = numer / denom
    both = jnp.concatenate([att, att], axis=0).T
    side = iota((TOK, 128), 1) < HD
    attl[...] = jnp.where(side, both, 0.0).astype(BF)
    atth[...] = jnp.where(side, 0.0, both).astype(BF)

    a_cps = []
    for s in range(1, NH):
        src = atth if s % 2 else attl
        start = pl.multiple_of(hpeer[s] * ROWS, ROWS)
        a_cps.append(
            send(src.at[pl.ds(start, ROWS)], arecv.at[s - 1], a_s.at[s - 1], a_r.at[s - 1], {"head": hpeer[s]})
        )
    for s in (1, 5, 13, 9, 3, 7, 15, 11):
        w_wait(s)
    mine = attl[pl.ds(pl.multiple_of(head * ROWS, ROWS), ROWS)]
    for cp in a_cps:
        cp.wait_recv()
    pairs = [mine + arecv[0]]
    for i in range(1, NH // 2):
        pairs.append(arecv[2 * i - 1] + arecv[2 * i])
    mixed = jnp.concatenate(pairs, axis=1)
    image = img_ref[blk * (TOK // BS) + head // (NH * BS // TOK)]
    gating = gate_ref[pl.ds(image, 1), :]
    projected = jnp.dot(mixed, wbuf[...], preferred_element_type=F32)
    out_ref[...] = (res_ref[...].astype(F32) + gating * projected).astype(BF)
    for cp in started:
        cp.wait_send()


def on_device(queries, key_rows, values, text_keys, text_values, block_image, gate_image, residual, w_out):
    vm = pl.BlockSpec(memory_space=pltpu.VMEM)
    sm = pl.BlockSpec(memory_space=pltpu.SMEM)
    dma = pltpu.SemaphoreType.DMA
    return pl.pallas_call(
        kernel,
        out_shape=jax.ShapeDtypeStruct((ROWS, D), BF),
        in_specs=[vm, vm, vm, vm, vm, sm, vm, vm, vm],
        out_specs=vm,
        scratch_shapes=[
            pltpu.VMEM((ZL, TOK, 128), BF),
            pltpu.VMEM((YL, HD, TOK), BF),
            pltpu.VMEM((YL, 128, TOK), BF),
            pltpu.VMEM((ZL + TSLOTS, TOK, 128), BF),
            pltpu.VMEM((ZL + TSLOTS, HD + 16, TOK), BF),
            pltpu.VMEM((YL, HD + 16, TOK), F32),
            pltpu.VMEM((YL, 8, TOK), F32),
            pltpu.VMEM((2, TSLOTS * TOK, HD), BF),
            pltpu.VMEM((3, HD, TOK), BF),
            pltpu.VMEM((3, HD, TOK), BF),
            pltpu.VMEM((3, 8, TOK), F32),
            pltpu.VMEM((3, 8, TOK), F32),
            pltpu.VMEM((TOK, 128), BF),
            pltpu.VMEM((TOK, 128), BF),
            pltpu.VMEM((NH - 1, ROWS, 128), BF),
            pltpu.VMEM((NH * HD, D), BF),
            dma((3,)), dma((3,)),
            dma((8,)), dma((8,)),
            dma((15,)), dma((16,)),
            dma((3,)), dma((3,)),
            dma((3,)), dma((3,)),
            dma((15,)), dma((15,)),
        ],
        compiler_params=pltpu.CompilerParams(
            collective_id=0, has_side_effects=True, vmem_limit_bytes=48 * 1024 * 1024
        ),
        name="joint_attention",
    )(queries, key_rows, values, text_keys, text_values, block_image, gate_image, residual, w_out)


def solution(mesh):
    placed = (
        P("blk", "head"),
        P("blk", "head"),
        P("blk", "head"),
        P(None, "head"),
        P(None, "head"),
        P(),
        P(),
        P(("blk", "head"), None),
        P("head", None),
    )
    return jax.shard_map(
        on_device, mesh=mesh, in_specs=placed, out_specs=P(("blk", "head"), None), check_vma=False
    )
```

```python
import functools
import math

import jax
import jax.numpy as jnp
from jax import lax
from jax.experimental import pallas as pl
from jax.experimental.pallas import tpu as pltpu
from jax.sharding import PartitionSpec as P

HD = 64
TEXT = 154
BS = 128
TOK = 512
YL = 4
ZL = 8
NH = 16
D = 1536
ROWS = TOK // NH
TSLOTS = 3
FAR = -(2.0**100)
RATE = math.log2(math.e) / math.sqrt(HD)
MESH = pl.DeviceIdType.MESH
BF = jnp.bfloat16
F32 = jnp.float32
NT = (((1,), (1,)), ((), ()))


def flip(index, mask, bits):
    total = 0
    for b in range(bits):
        bit = (index // (1 << b)) % 2
        total = total + (1 << b) * ((1 - bit) if (mask >> b) & 1 else bit)
    return total


def iota(shape, dim):
    return lax.broadcasted_iota(jnp.int32, shape, dim)


def kernel(
    q_hbm, k_hbm, v_hbm, tk_hbm, tv_hbm, img_ref, gate_hbm, res_hbm, w_hbm,
    out_ref,
    kv, qt, tk_ref, tv_ref, gate_ref, res_ref, qa, ka, va, acc, mx, tpad, osend, orecv, ssend, srecv, attl, atth, arecv, wbuf,
    q_s, q_r, kv_s, kv_r, w_s, w_r, o_s, o_r, st_s, st_r, a_s, a_r, in_s,
):
    blk = lax.axis_index("blk")
    head = lax.axis_index("head")
    z = blk // YL
    y = blk % YL
    zright = ((z + 1) % ZL) * YL + y
    zleft = ((z + ZL - 1) % ZL) * YL + y
    ypeer = [z * YL + flip(y, c, 2) for c in range(YL)]
    hpeer = [flip(head, s, 4) for s in range(NH)]

    barrier = pltpu.get_barrier_semaphore()
    for other in (zright, zleft, ypeer[1], ypeer[2], ypeer[3]):
        pl.semaphore_signal(barrier, inc=1, device_id={"blk": other}, device_id_type=MESH)
    for s in range(1, NH):
        pl.semaphore_signal(barrier, inc=1, device_id={"head": hpeer[s]}, device_id_type=MESH)

    loads = [
        pltpu.make_async_copy(src, dst, in_s.at[n])
        for n, (src, dst) in enumerate((
            (q_hbm, qt.at[0]),
            (k_hbm, kv.at[0, pl.ds(0, HD)]),
            (v_hbm, kv.at[0, pl.ds(HD, HD)]),
            (w_hbm, wbuf.at[pl.ds(0, HD)]),
            (tk_hbm, tk_ref),
            (tv_hbm, tv_ref),
            (gate_hbm, gate_ref),
            (res_hbm, res_ref),
        ))
    ]
    for cp in loads:
        cp.start()

    for cp in loads[:4]:
        cp.wait()
    with jax.named_scope("barrier"):
        pl.semaphore_wait(barrier, 5 + NH - 1)

    started = []

    def send(src, dst, ssem, rsem, dev):
        copy = pltpu.make_async_remote_copy(
            src_ref=src, dst_ref=dst, send_sem=ssem, recv_sem=rsem,
            device_id=dev, device_id_type=MESH,
        )
        copy.start()
        started.append(copy)
        return copy

    def q_copy(c):
        return send(qt.at[0], qt.at[c], q_s.at[c - 1], q_r.at[c - 1], {"blk": ypeer[c]})

    def kv_right(step):
        src = 0 if step == 1 else ZL - (step - 1)
        dst = ZL - step
        rows = pl.ds(0, HD) if step == 4 else pl.ds(0, 2 * HD)
        return send(kv.at[src, rows], kv.at[dst, rows], kv_s.at[step - 1], kv_r.at[step - 1], {"blk": zright})

    def kv_left(step):
        rows = pl.ds(HD, HD) if step == 4 else pl.ds(0, 2 * HD)
        return send(kv.at[step - 1, rows], kv.at[step, rows], kv_s.at[step + 3], kv_r.at[step + 3], {"blk": zleft})

    w_count = [0]

    def w_copy(origin, to):
        src = wbuf.at[pl.ds(origin * HD, HD)]
        slot = origin ^ to
        k = w_count[0]
        w_count[0] += 1
        return send(src, wbuf.at[pl.ds(slot * HD, HD)], w_s.at[k], w_r.at[slot], {"head": hpeer[to]})

    def w_wait(slot):
        part = wbuf.at[pl.ds(slot * HD, HD)]
        pltpu.make_async_remote_copy(
            src_ref=part, dst_ref=part, send_sem=w_s.at[0], recv_sem=w_r.at[slot],
            device_id={"head": hpeer[1]}, device_id_type=MESH,
        ).wait_recv()

    q_cps = [None] + [q_copy(c) for c in (1, 2, 3)]
    r_cps = {1: kv_right(1)}
    l_cps = {1: kv_left(1)}
    w_copy(0, 2)
    for s in (4, 12, 8):
        w_copy(0, s)
    w_copy(0, 1)

    def fill_keys(slot, first_block):
        row = iota((HD, BS), 0)
        gaps = []
        for b in range(TOK // BS):
            image = img_ref[first_block + b]
            gaps.append(jnp.where((row < 8) & (row != image), FAR, 0.0))
        wide = jnp.concatenate([kv[slot, 0:HD].astype(F32), jnp.concatenate(gaps, axis=1)], axis=0)
        ka[slot] = wide.T.astype(BF)
        va[slot, 0:HD] = kv[slot, HD : 2 * HD]
        va[slot, HD : HD + 16] = jnp.ones((16, TOK), BF)

    def fill_queries(c):
        qa[c, 0:HD] = qt[c]
        first = ypeer[c] * (TOK // BS)
        for b in range(TOK // BS):
            image = img_ref[first + b]
            hot = (iota((16, BS), 0) == image).astype(F32)
            qa[c, HD : HD + 16, b * BS : (b + 1) * BS] = hot.astype(BF)
        qa[c, HD + 16 : 128] = jnp.zeros((128 - HD - 16, TOK), BF)

    def process(slot, c):
        keys = ka[slot]
        vals = va[slot]
        for part in range(2):
            cols = slice(part * 256, part * 256 + 256)
            sc = jnp.dot(keys, qa[c, :, cols], preferred_element_type=F32)
            old = mx[c, 0:1, cols]
            new = jnp.maximum(old, jnp.max(sc, axis=0, keepdims=True))
            pr = jnp.exp2((sc - new) * RATE).astype(BF)
            shrink = jnp.exp2((old - new) * RATE)
            upd = jnp.dot(vals, pr, preferred_element_type=F32)
            acc[c, :, cols] = acc[c, :, cols] * shrink + upd
            mx[c, 0:1, cols] = new

    for c in range(YL):
        acc[c] = jnp.zeros((HD + 16, TOK), F32)
        mx[c] = jnp.full((8, TOK), FAR, F32)

    fill_queries(0)
    loads[4].wait()
    loads[5].wait()
    ntext = tk_ref.shape[1]
    edge = (TSLOTS - 1) * TOK
    for n, ref in ((0, tk_ref), (1, tv_ref)):
        tpad[n, :, edge:] = jnp.zeros((HD, TOK), BF)
        tpad[n, :, 0:ntext] = ref[...]
    for t in range(TSLOTS):
        row = iota((HD, TOK), 0)
        col = iota((HD, TOK), 1) + t * TOK
        inside = (col >= row * TEXT) & (col < (row + 1) * TEXT)
        gap = jnp.where((row < 8) & jnp.logical_not(inside), FAR, 0.0)
        span = slice(t * TOK, (t + 1) * TOK)
        wide = jnp.concatenate([tpad[0, :, span].astype(F32), gap], axis=0)
        ka[ZL + t] = wide.T.astype(BF)
        va[ZL + t, 0:HD] = tpad[1, :, span]
        va[ZL + t, HD : HD + 16] = jnp.ones((16, TOK), BF)

    fill_keys(0, blk * (TOK // BS))

    def own_step(t, carry):
        slot = (ZL + t) % (ZL + TSLOTS)
        process(slot, 0)
        return carry

    with jax.named_scope("own"):
        lax.fori_loop(0, TSLOTS + 1, own_step, 0)

    with jax.named_scope("qwait"):
        for c in (1, 2, 3):
            q_cps[c].wait_recv()
    for c in (1, 2, 3):
        fill_queries(c)

    def first_step(c, carry):
        process(0, c)
        return carry

    lax.fori_loop(1, YL, first_step, 0)

    def origin_block(slot):
        return (((z + slot) % ZL) * YL + y) * (TOK // BS)

    for step in (1, 2, 3):
        with jax.named_scope(f"kvwait{step}"):
            r_cps[step].wait_recv()
            r_cps[step + 1] = kv_right(step + 1)
            l_cps[step].wait_recv()
            l_cps[step + 1] = kv_left(step + 1)
        fill_keys(ZL - step, origin_block(ZL - step))
        fill_keys(step, origin_block(step))

        def mid_step(t, carry, step=step):
            side = t // YL
            slot = step + side * (ZL - 2 * step)
            process(slot, t % YL)
            return carry

        lax.fori_loop(0, 2 * YL, mid_step, 0)
        if step == 1:
            for s in (4, 12, 8):
                with jax.named_scope("wxwait"):
                    w_wait(s)
                w_copy(s, 1)
        if step == 2:
            with jax.named_scope("wywait"):
                w_wait(2)
            for s in (4, 12, 8):
                w_copy(2, s)
            w_copy(2, 1)

    with jax.named_scope("kvwait4"):
        r_cps[4].wait_recv()
        l_cps[4].wait_recv()
    fill_keys(4, origin_block(4))
    o_cps = [None] * YL
    st_cps = [None] * YL
    for c in (3, 2, 1):
        process(4, c)
        osend[c - 1] = acc[c, 0:HD].astype(BF)
        ssend[c - 1, 0:1] = mx[c, 0:1]
        ssend[c - 1, 1:2] = acc[c, HD : HD + 1]
        ssend[c - 1, 2:8] = jnp.zeros((6, TOK), F32)
        dev = {"blk": ypeer[c]}
        o_cps[c] = send(osend.at[c - 1], orecv.at[c - 1], o_s.at[c - 1], o_r.at[c - 1], dev)
        st_cps[c] = send(ssend.at[c - 1], srecv.at[c - 1], st_s.at[c - 1], st_r.at[c - 1], dev)
    process(4, 0)
    for s in (6, 14, 10):
        with jax.named_scope("wxwait2"):
            w_wait(s)
        w_copy(s, 1)
    with jax.named_scope("owait"):
        for c in (1, 2, 3):
            o_cps[c].wait_recv()
            st_cps[c].wait_recv()

    maxes = [mx[0, 0:1]] + [srecv[c - 1, 0:1] for c in (1, 2, 3)]
    sums = [acc[0, HD : HD + 1]] + [srecv[c - 1, 1:2] for c in (1, 2, 3)]
    top = functools.reduce(jnp.maximum, maxes)
    scales = [jnp.exp2((m - top) * RATE) for m in maxes]
    denom = functools.reduce(jnp.add, [s * l for s, l in zip(scales, sums)])
    numer = acc[0, 0:HD] * scales[0]
    for c in (1, 2, 3):
        numer = numer + orecv[c - 1].astype(F32) * scales[c]
    att = numer / denom
    both = jnp.concatenate([att, att], axis=0).T
    side = iota((TOK, 128), 1) < HD
    attl[...] = jnp.where(side, both, 0.0).astype(BF)
    atth[...] = jnp.where(side, 0.0, both).astype(BF)

    a_cps = []
    for s in range(1, NH):
        src = atth if s % 2 else attl
        start = pl.multiple_of(hpeer[s] * ROWS, ROWS)
        a_cps.append(
            send(src.at[pl.ds(start, ROWS)], arecv.at[s - 1], a_s.at[s - 1], a_r.at[s - 1], {"head": hpeer[s]})
        )
    with jax.named_scope("wcwait"):
        for s in (1, 5, 13, 9, 3, 7, 15, 11):
            w_wait(s)
    mine = attl[pl.ds(pl.multiple_of(head * ROWS, ROWS), ROWS)]
    with jax.named_scope("await"):
        for cp in a_cps:
            cp.wait_recv()
    loads[6].wait()
    loads[7].wait()
    pairs = [mine + arecv[0]]
    for i in range(1, NH // 2):
        pairs.append(arecv[2 * i - 1] + arecv[2 * i])
    mixed = jnp.concatenate(pairs, axis=1)
    image = img_ref[blk * (TOK // BS) + head // (NH * BS // TOK)]
    gating = gate_ref[pl.ds(image, 1), :]
    projected = jnp.dot(mixed, wbuf[...], preferred_element_type=F32)
    out_ref[...] = (res_ref[...].astype(F32) + gating * projected).astype(BF)
    with jax.named_scope("sendwait"):
        for cp in started:
            cp.wait_send()


def on_device(queries, key_rows, values, text_keys, text_values, block_image, gate_image, residual, w_out):
    vm = pl.BlockSpec(memory_space=pltpu.VMEM)
    hb = pl.BlockSpec(memory_space=pl.ANY)
    sm = pl.BlockSpec(memory_space=pltpu.SMEM)
    dma = pltpu.SemaphoreType.DMA
    return pl.pallas_call(
        kernel,
        out_shape=jax.ShapeDtypeStruct((ROWS, D), BF),
        in_specs=[hb, hb, hb, hb, hb, sm, hb, hb, hb],
        out_specs=vm,
        scratch_shapes=[
            pltpu.VMEM((ZL, 2 * HD, TOK), BF),
            pltpu.VMEM((YL, HD, TOK), BF),
            pltpu.VMEM((HD, text_keys.shape[0]), BF),
            pltpu.VMEM((HD, text_keys.shape[0]), BF),
            pltpu.VMEM(gate_image.shape, F32),
            pltpu.VMEM((ROWS, D), BF),
            pltpu.VMEM((YL, 128, TOK), BF),
            pltpu.VMEM((ZL + TSLOTS, TOK, 128), BF),
            pltpu.VMEM((ZL + TSLOTS, HD + 16, TOK), BF),
            pltpu.VMEM((YL, HD + 16, TOK), F32),
            pltpu.VMEM((YL, 8, TOK), F32),
            pltpu.VMEM((2, HD, TSLOTS * TOK), BF),
            pltpu.VMEM((3, HD, TOK), BF),
            pltpu.VMEM((3, HD, TOK), BF),
            pltpu.VMEM((3, 8, TOK), F32),
            pltpu.VMEM((3, 8, TOK), F32),
            pltpu.VMEM((TOK, 128), BF),
            pltpu.VMEM((TOK, 128), BF),
            pltpu.VMEM((NH - 1, ROWS, 128), BF),
            pltpu.VMEM((NH * HD, D), BF),
            dma((3,)), dma((3,)),
            dma((8,)), dma((8,)),
            dma((15,)), dma((16,)),
            dma((3,)), dma((3,)),
            dma((3,)), dma((3,)),
            dma((15,)), dma((15,)),
            dma((8,)),
        ],
        compiler_params=pltpu.CompilerParams(
            collective_id=0, has_side_effects=True, vmem_limit_bytes=60 * 1024 * 1024
        ),
        name="joint_attention",
    )(
        queries.T, key_rows.T, values.T, text_keys.T, text_values.T,
        block_image, gate_image, residual, w_out,
    )


def solution(mesh):
    placed = (
        P("blk", "head"),
        P("blk", "head"),
        P("blk", "head"),
        P(None, "head"),
        P(None, "head"),
        P(),
        P(),
        P(("blk", "head"), None),
        P("head", None),
    )
    return jax.shard_map(
        on_device, mesh=mesh, in_specs=placed, out_specs=P(("blk", "head"), None), check_vma=False
    )
```

```python
import functools
import math

import jax
import jax.numpy as jnp
from jax import lax
from jax.experimental import pallas as pl
from jax.experimental.pallas import tpu as pltpu
from jax.sharding import PartitionSpec as P

HD = 64
TEXT = 154
BS = 128
TOK = 512
YL = 4
ZL = 8
NH = 16
D = 1536
ROWS = TOK // NH
TSLOTS = 3
FAR = -(2.0**100)
RATE = math.log2(math.e) / math.sqrt(HD)
MESH = pl.DeviceIdType.MESH
BF = jnp.bfloat16
F32 = jnp.float32
NT = (((1,), (1,)), ((), ()))


def flip(index, mask, bits):
    total = 0
    for b in range(bits):
        bit = (index // (1 << b)) % 2
        total = total + (1 << b) * ((1 - bit) if (mask >> b) & 1 else bit)
    return total


def iota(shape, dim):
    return lax.broadcasted_iota(jnp.int32, shape, dim)


def kernel(
    q_hbm, k_hbm, v_hbm, tk_hbm, tv_hbm, img_hbm, gate_hbm, res_hbm, w_hbm,
    out_ref,
    img_ref, kv, qt, tk_ref, tv_ref, gate_ref, res_ref, qa, ka, va, acc, mx, tpad, s0, s1, osend, orecv, ssend, srecv, attl, atth, arecv, wbuf,
    q_s, q_r, kv_s, kv_r, w_s, w_r, o_s, o_r, st_s, st_r, a_s, a_r, in_s,
):
    blk = lax.axis_index("blk")
    head = lax.axis_index("head")
    z = blk // YL
    y = blk % YL
    zright = ((z + 1) % ZL) * YL + y
    zleft = ((z + ZL - 1) % ZL) * YL + y
    ypeer = [z * YL + flip(y, c, 2) for c in range(YL)]
    hpeer = [flip(head, s, 4) for s in range(NH)]

    barrier = pltpu.get_barrier_semaphore()
    for other in (zright, zleft, ypeer[1], ypeer[2], ypeer[3]):
        pl.semaphore_signal(barrier, inc=1, device_id={"blk": other}, device_id_type=MESH)
    for s in range(1, NH):
        pl.semaphore_signal(barrier, inc=1, device_id={"head": hpeer[s]}, device_id_type=MESH)

    loads = [
        pltpu.make_async_copy(src, dst, in_s.at[n])
        for n, (src, dst) in enumerate((
            (img_hbm, img_ref),
            (q_hbm, qt.at[0]),
            (k_hbm, kv.at[0, pl.ds(0, HD)]),
            (v_hbm, kv.at[0, pl.ds(HD, HD)]),
            (w_hbm, wbuf.at[pl.ds(0, HD)]),
            (tk_hbm, tk_ref),
            (tv_hbm, tv_ref),
            (gate_hbm, gate_ref),
            (res_hbm, res_ref),
        ))
    ]
    for cp in loads:
        cp.start()

    started = []

    def send(src, dst, ssem, rsem, dev):
        copy = pltpu.make_async_remote_copy(
            src_ref=src, dst_ref=dst, send_sem=ssem, recv_sem=rsem,
            device_id=dev, device_id_type=MESH,
        )
        copy.start()
        started.append(copy)
        return copy

    def q_copy(c):
        return send(qt.at[0], qt.at[c], q_s.at[c - 1], q_r.at[c - 1], {"blk": ypeer[c]})

    kv_cps = {}

    def kv_send(kind, step):
        src = step - 1 if kind in ("lk", "lv") or step == 1 else ZL - (step - 1)
        dst = step if kind in ("lk", "lv") else ZL - step
        k = {"rk": 0, "rv": 4, "lk": 7, "lv": 10}[kind] + step - 1
        rows = pl.ds(0 if kind in ("rk", "lk") else HD, HD)
        dev = {"blk": zleft if kind in ("lk", "lv") else zright}
        kv_cps[kind, step] = send(kv.at[src, rows], kv.at[dst, rows], kv_s.at[k], kv_r.at[k], dev)

    def kv_hop(step):
        for kind, last in (("rk", 4), ("lk", 3), ("rv", 3), ("lv", 4)):
            if (kind, step) in kv_cps:
                kv_cps[kind, step].wait_recv()
                if step < last:
                    kv_send(kind, step + 1)

    w_count = [0]

    def w_part(slot, half):
        if half is None:
            return wbuf.at[pl.ds(slot * HD, HD)]
        return wbuf.at[pl.ds(slot * HD + half * (HD // 2), HD // 2)]

    def w_sem(slot, half):
        return w_r.at[slot if half in (None, 0) else NH + slot]

    def w_copy(origin, to, half=None):
        slot = origin ^ to
        k = w_count[0]
        w_count[0] += 1
        return send(w_part(origin, half), w_part(slot, half), w_s.at[k], w_sem(slot, half), {"head": hpeer[to]})

    def w_wait(slot, half=None):
        part = w_part(slot, half)
        pltpu.make_async_remote_copy(
            src_ref=part, dst_ref=part, send_sem=w_s.at[0], recv_sem=w_sem(slot, half),
            device_id={"head": hpeer[1]}, device_id_type=MESH,
        ).wait_recv()

    def fill_keys(slot, first_block):
        row = iota((HD, BS), 0)
        gaps = []
        for b in range(TOK // BS):
            image = img_ref[first_block + b]
            gaps.append(jnp.where((row < 8) & (row != image), FAR, 0.0))
        wide = jnp.concatenate([kv[slot, 0:HD].astype(F32), jnp.concatenate(gaps, axis=1)], axis=0)
        ka[slot] = wide.T.astype(BF)
        va[slot, 0:HD] = kv[slot, HD : 2 * HD]
        va[slot, HD : HD + 16] = jnp.ones((16, TOK), BF)

    def fill_queries(c):
        qa[c, 0:HD] = qt[c]
        first = ypeer[c] * (TOK // BS)
        for b in range(TOK // BS):
            image = img_ref[first + b]
            hot = (iota((16, BS), 0) == image).astype(F32)
            qa[c, HD : HD + 16, b * BS : (b + 1) * BS] = hot.astype(BF)
        qa[c, HD + 16 : 128] = jnp.zeros((128 - HD - 16, TOK), BF)

    seen = set()
    pending = []
    turn = [0]

    def scores(slot, c, n, buf):
        sc = jnp.dot(ka[slot, 0:n], qa[c], preferred_element_type=F32)
        buf[0:n] = sc
        buf[TOK : TOK + 8] = jnp.max(sc.reshape(n // 8, 8, TOK), axis=0)

    def soften(slot, c, n, buf):
        new = jnp.max(buf[TOK : TOK + 8], axis=0, keepdims=True)
        if c in seen:
            old = mx[c, 0:1]
            new = jnp.maximum(old, new)
            shrink = jnp.exp2((old - new) * RATE)
        pr = jnp.exp2((buf[0:n] - new) * RATE).astype(BF)
        upd = jnp.dot(va[slot, :, 0:n], pr, preferred_element_type=F32)
        if c in seen:
            acc[c] = acc[c] * shrink + upd
        else:
            acc[c] = upd
        mx[c, 0:1] = new
        seen.add(c)

    def flush():
        while pending:
            soften(*pending.pop(0))

    def steps(*pairs):
        for slot, c in pairs:
            n = tail if slot == ZL + TSLOTS - 1 else TOK
            buf = (s0, s1)[turn[0] % 2]
            turn[0] += 1
            scores(slot, c, n, buf)
            flush()
            pending.append((slot, c, n, buf))

    def origin_block(slot):
        return (((z + slot) % ZL) * YL + y) * (TOK // BS)

    o_cps = [None] * YL
    st_cps = [None] * YL

    def send_part(c):
        osend[c - 1] = acc[c, 0:HD].astype(BF)
        for a in range(4):
            ssend[c - 1, a : a + 1] = mx[c, 0:1, a * 128 : (a + 1) * 128]
            ssend[c - 1, 4 + a : 5 + a] = acc[c, HD : HD + 1, a * 128 : (a + 1) * 128]
        dev = {"blk": ypeer[c]}
        o_cps[c] = send(osend.at[c - 1], orecv.at[c - 1], o_s.at[c - 1], o_r.at[c - 1], dev)
        st_cps[c] = send(ssend.at[c - 1], srecv.at[c - 1], st_s.at[c - 1], st_r.at[c - 1], dev)

    ntext = tk_hbm.shape[1]
    edge = (TSLOTS - 1) * TOK
    tail = -(-(ntext - edge) // 128) * 128
    for cp in loads[:4]:
        cp.wait()
    fill_queries(0)
    fill_keys(0, blk * (TOK // BS))

    with jax.named_scope("barrier"):
        pl.semaphore_wait(barrier, 5 + NH - 1)

    q_cps = [None] + [q_copy(c) for c in (1, 2, 3)]
    for kind in ("rk", "lk", "rv", "lv"):
        kv_send(kind, 1)
    loads[4].wait()
    for s in (4, 12, 8):
        w_copy(0, s)
    w_copy(0, 1)

    loads[5].wait()
    loads[6].wait()
    for n, ref in ((0, tk_ref), (1, tv_ref)):
        tpad[n, :, edge:] = jnp.zeros((HD, TOK), BF)
        tpad[n, :, 0:ntext] = ref[...]
    for t in range(TSLOTS):
        row = iota((HD, TOK), 0)
        col = iota((HD, TOK), 1) + t * TOK
        inside = (col >= row * TEXT) & (col < (row + 1) * TEXT)
        gap = jnp.where((row < 8) & jnp.logical_not(inside), FAR, 0.0)
        span = slice(t * TOK, (t + 1) * TOK)
        wide = jnp.concatenate([tpad[0, :, span].astype(F32), gap], axis=0)
        ka[ZL + t] = wide.T.astype(BF)
        va[ZL + t, 0:HD] = tpad[1, :, span]
        va[ZL + t, HD : HD + 16] = jnp.ones((16, TOK), BF)

    with jax.named_scope("text"):
        steps((8, 0), (9, 0), (10, 0), (0, 0))
        flush()
    with jax.named_scope("qwait1"):
        q_cps[1].wait_recv()
    fill_queries(1)
    steps((0, 1))
    flush()
    with jax.named_scope("kvwait1"):
        kv_hop(1)
    w_copy(0, 2, 0)
    fill_keys(7, origin_block(7))
    fill_keys(1, origin_block(1))
    steps((7, 0), (1, 0), (7, 1), (1, 1))
    flush()
    with jax.named_scope("qwait2"):
        q_cps[2].wait_recv()
    w_copy(0, 2, 1)
    fill_queries(2)
    steps((0, 2), (7, 2), (1, 2))
    flush()
    with jax.named_scope("kvwait2"):
        kv_hop(2)
    fill_keys(6, origin_block(6))
    fill_keys(2, origin_block(2))
    steps((6, 0), (2, 0), (6, 1), (2, 1), (6, 2), (2, 2))
    flush()
    with jax.named_scope("qwait3"):
        q_cps[3].wait_recv()
    fill_queries(3)
    steps((0, 3), (7, 3), (1, 3))
    flush()
    with jax.named_scope("kvwait3"):
        kv_hop(3)
    fill_keys(5, origin_block(5))
    fill_keys(3, origin_block(3))
    steps((6, 3), (2, 3), (5, 0), (3, 0))
    flush()
    with jax.named_scope("wywait"):
        w_wait(2, 0)
    for s in (4, 12, 8):
        w_copy(2, s, 0)
    for s in (4, 12, 8):
        w_wait(s)
        w_copy(s, 1)
    with jax.named_scope("kvwait4"):
        kv_hop(4)
    fill_keys(4, origin_block(4))
    with jax.named_scope("last"):
        steps((5, 3), (3, 3), (4, 3), (5, 2))
        send_part(3)
        steps((3, 2), (4, 2), (5, 1))
        send_part(2)
        steps((3, 1), (4, 1), (4, 0))
        send_part(1)
        flush()
    with jax.named_scope("wywait2"):
        w_wait(2, 1)
    for s in (4, 12, 8):
        w_copy(2, s, 1)
    w_copy(2, 1)
    with jax.named_scope("owait"):
        for c in (1, 2, 3):
            o_cps[c].wait_recv()
            st_cps[c].wait_recv()

    def row_of(ref, c, first):
        return jnp.concatenate([ref[c - 1, first + a : first + a + 1] for a in range(4)], axis=1)

    maxes = [mx[0, 0:1]] + [row_of(srecv, c, 0) for c in (1, 2, 3)]
    sums = [acc[0, HD : HD + 1]] + [row_of(srecv, c, 4) for c in (1, 2, 3)]
    top = functools.reduce(jnp.maximum, maxes)
    scales = [jnp.exp2((m - top) * RATE) for m in maxes]
    denom = functools.reduce(jnp.add, [s * l for s, l in zip(scales, sums)])
    numer = acc[0, 0:HD] * scales[0]
    for c in (1, 2, 3):
        numer = numer + orecv[c - 1].astype(F32) * scales[c]
    att = numer / denom
    both = jnp.concatenate([att, att], axis=0).T
    side = iota((TOK, 128), 1) < HD
    attl[...] = jnp.where(side, both, 0.0).astype(BF)
    atth[...] = jnp.where(side, 0.0, both).astype(BF)

    a_cps = []
    for s in range(1, NH):
        src = atth if s % 2 else attl
        start = pl.multiple_of(hpeer[s] * ROWS, ROWS)
        a_cps.append(
            send(src.at[pl.ds(start, ROWS)], arecv.at[s - 1], a_s.at[s - 1], a_r.at[s - 1], {"head": hpeer[s]})
        )
    for s in (6, 14, 10):
        with jax.named_scope("wxwait2"):
            w_wait(s, 0)
            w_wait(s, 1)
        w_copy(s, 1)
    mine = attl[pl.ds(pl.multiple_of(head * ROWS, ROWS), ROWS)]
    with jax.named_scope("await"):
        for cp in a_cps:
            cp.wait_recv()
    loads[7].wait()
    loads[8].wait()
    with jax.named_scope("wcwait"):
        for s in (1, 5, 13, 9, 3, 7, 15, 11):
            w_wait(s)
    pairs = [mine + arecv[0]]
    for i in range(1, NH // 2):
        pairs.append(arecv[2 * i - 1] + arecv[2 * i])
    mixed = jnp.concatenate(pairs, axis=1)
    image = img_ref[blk * (TOK // BS) + head // (NH * BS // TOK)]
    gating = gate_ref[pl.ds(image, 1), :]
    projected = jnp.dot(mixed, wbuf[...], preferred_element_type=F32)
    out_ref[...] = (res_ref[...].astype(F32) + gating * projected).astype(BF)
    with jax.named_scope("sendwait"):
        for cp in started:
            cp.wait_send()


def on_device(queries, key_rows, values, text_keys, text_values, block_image, gate_image, residual, w_out):
    vm = pl.BlockSpec(memory_space=pltpu.VMEM)
    hb = pl.BlockSpec(memory_space=pl.ANY)
    dma = pltpu.SemaphoreType.DMA
    return pl.pallas_call(
        kernel,
        out_shape=jax.ShapeDtypeStruct((ROWS, D), BF),
        in_specs=[hb] * 9,
        out_specs=vm,
        scratch_shapes=[
            pltpu.SMEM(block_image.shape, jnp.int32),
            pltpu.VMEM((ZL, 2 * HD, TOK), BF),
            pltpu.VMEM((YL, HD, TOK), BF),
            pltpu.VMEM((HD, text_keys.shape[0]), BF),
            pltpu.VMEM((HD, text_keys.shape[0]), BF),
            pltpu.VMEM(gate_image.shape, F32),
            pltpu.VMEM((ROWS, D), BF),
            pltpu.VMEM((YL, 128, TOK), BF),
            pltpu.VMEM((ZL + TSLOTS, TOK, 128), BF),
            pltpu.VMEM((ZL + TSLOTS, HD + 16, TOK), BF),
            pltpu.VMEM((YL, HD + 16, TOK), F32),
            pltpu.VMEM((YL, 8, TOK), F32),
            pltpu.VMEM((2, HD, TSLOTS * TOK), BF),
            pltpu.VMEM((TOK + 8, TOK), F32),
            pltpu.VMEM((TOK + 8, TOK), F32),
            pltpu.VMEM((3, HD, TOK), BF),
            pltpu.VMEM((3, HD, TOK), BF),
            pltpu.VMEM((3, 8, 128), F32),
            pltpu.VMEM((3, 8, 128), F32),
            pltpu.VMEM((TOK, 128), BF),
            pltpu.VMEM((TOK, 128), BF),
            pltpu.VMEM((NH - 1, ROWS, 128), BF),
            pltpu.VMEM((NH * HD, D), BF),
            dma((3,)), dma((3,)),
            dma((14,)), dma((14,)),
            dma((19,)), dma((32,)),
            dma((3,)), dma((3,)),
            dma((3,)), dma((3,)),
            dma((15,)), dma((15,)),
            dma((9,)),
        ],
        compiler_params=pltpu.CompilerParams(
            collective_id=0, has_side_effects=True, vmem_limit_bytes=60 * 1024 * 1024
        ),
        name="joint_attention",
    )(
        queries.T, key_rows.T, values.T, text_keys.T, text_values.T,
        block_image, gate_image, residual, w_out,
    )


def solution(mesh):
    placed = (
        P("blk", "head"),
        P("blk", "head"),
        P("blk", "head"),
        P(None, "head"),
        P(None, "head"),
        P(),
        P(),
        P(("blk", "head"), None),
        P("head", None),
    )
    return jax.shard_map(
        on_device, mesh=mesh, in_specs=placed, out_specs=P(("blk", "head"), None), check_vma=False
    )
```

```python
import functools
import math

import jax
import jax.numpy as jnp
from jax import lax
from jax.experimental import pallas as pl
from jax.experimental.pallas import tpu as pltpu
from jax.sharding import PartitionSpec as P

HD = 64
TEXT = 154
BS = 128
TOK = 512
YL = 4
ZL = 8
NH = 16
D = 1536
ROWS = TOK // NH
TSLOTS = 3
FAR = -(2.0**100)
RATE = math.log2(math.e) / math.sqrt(HD)
MESH = pl.DeviceIdType.MESH
BF = jnp.bfloat16
F32 = jnp.float32
NT = (((1,), (1,)), ((), ()))


def flip(index, mask, bits):
    total = 0
    for b in range(bits):
        bit = (index // (1 << b)) % 2
        total = total + (1 << b) * ((1 - bit) if (mask >> b) & 1 else bit)
    return total


def iota(shape, dim):
    return lax.broadcasted_iota(jnp.int32, shape, dim)


def kernel(
    q_hbm, k_hbm, v_hbm, tk_hbm, tv_hbm, img_hbm, gate_hbm, res_hbm, w_hbm,
    out_ref,
    img_ref, kv, qt, tk_ref, tv_ref, gate_ref, res_ref, qa, ka, va, acc, mx, tpad, s0, s1, osend, orecv, ssend, srecv, packed, arecv, wbuf,
    q_s, q_r, kv_s, kv_r, w_s, w_r, o_s, o_r, st_s, st_r, a_s, a_r, in_s,
):
    blk = lax.axis_index("blk")
    head = lax.axis_index("head")
    z = blk // YL
    y = blk % YL
    zright = ((z + 1) % ZL) * YL + y
    zleft = ((z + ZL - 1) % ZL) * YL + y
    ypeer = [z * YL + flip(y, c, 2) for c in range(YL)]
    hpeer = [flip(head, s, 4) for s in range(NH)]

    barrier = pltpu.get_barrier_semaphore()
    for other in (zright, zleft, ypeer[1], ypeer[2], ypeer[3]):
        pl.semaphore_signal(barrier, inc=1, device_id={"blk": other}, device_id_type=MESH)
    for s in range(1, NH):
        pl.semaphore_signal(barrier, inc=1, device_id={"head": hpeer[s]}, device_id_type=MESH)

    loads = [
        pltpu.make_async_copy(src, dst, in_s.at[n])
        for n, (src, dst) in enumerate((
            (img_hbm, img_ref),
            (q_hbm, qt.at[0]),
            (k_hbm, kv.at[0, pl.ds(0, HD)]),
            (v_hbm, kv.at[0, pl.ds(HD, HD)]),
            (w_hbm, wbuf.at[pl.ds(0, HD)]),
            (tk_hbm, tk_ref),
            (tv_hbm, tv_ref),
            (gate_hbm, gate_ref),
            (res_hbm, res_ref),
        ))
    ]
    for cp in loads:
        cp.start()

    started = []

    def send(src, dst, ssem, rsem, dev):
        copy = pltpu.make_async_remote_copy(
            src_ref=src, dst_ref=dst, send_sem=ssem, recv_sem=rsem,
            device_id=dev, device_id_type=MESH,
        )
        copy.start()
        started.append(copy)
        return copy

    def q_copy(c):
        return send(qt.at[0], qt.at[c], q_s.at[c - 1], q_r.at[c - 1], {"blk": ypeer[c]})

    kv_cps = {}

    def kv_send(kind, step):
        src = step - 1 if kind in ("lk", "lv") or step == 1 else ZL - (step - 1)
        dst = step if kind in ("lk", "lv") else ZL - step
        k = {"rk": 0, "rv": 4, "lk": 7, "lv": 10}[kind] + step - 1
        rows = pl.ds(0 if kind in ("rk", "lk") else HD, HD)
        dev = {"blk": zleft if kind in ("lk", "lv") else zright}
        kv_cps[kind, step] = send(kv.at[src, rows], kv.at[dst, rows], kv_s.at[k], kv_r.at[k], dev)

    def kv_hop(part, step):
        for kind in ("r" + part, "l" + part):
            if (kind, step) in kv_cps:
                kv_cps[kind, step].wait_recv()
                if (kind, step + 1) not in kv_cps and step < {"rk": 4, "lk": 3, "rv": 3, "lv": 4}[kind]:
                    kv_send(kind, step + 1)

    w_count = [0]

    def w_part(slot, half):
        if half is None:
            return wbuf.at[pl.ds(slot * HD, HD)]
        return wbuf.at[pl.ds(slot * HD + half * (HD // 2), HD // 2)]

    def w_sem(slot, half):
        return w_r.at[slot if half in (None, 0) else NH + slot]

    def w_copy(origin, to, half=None):
        slot = origin ^ to
        k = w_count[0]
        w_count[0] += 1
        return send(w_part(origin, half), w_part(slot, half), w_s.at[k], w_sem(slot, half), {"head": hpeer[to]})

    def w_wait(slot, half=None):
        part = w_part(slot, half)
        pltpu.make_async_remote_copy(
            src_ref=part, dst_ref=part, send_sem=w_s.at[0], recv_sem=w_sem(slot, half),
            device_id={"head": hpeer[1]}, device_id_type=MESH,
        ).wait_recv()

    def fill_keys(slot, first_block):
        row = iota((HD, BS), 0)
        gaps = []
        for b in range(TOK // BS):
            image = img_ref[first_block + b]
            gaps.append(jnp.where((row < 8) & (row != image), FAR, 0.0))
        wide = jnp.concatenate([kv[slot, 0:HD].astype(F32), jnp.concatenate(gaps, axis=1)], axis=0)
        ka[slot] = wide.T.astype(BF)
        va[slot, 0:HD] = kv[slot, HD : 2 * HD]
        va[slot, HD : HD + 16] = jnp.ones((16, TOK), BF)

    def fill_queries(c):
        qa[c, 0:HD] = qt[c]
        first = ypeer[c] * (TOK // BS)
        for b in range(TOK // BS):
            image = img_ref[first + b]
            hot = (iota((16, BS), 0) == image).astype(F32)
            qa[c, HD : HD + 16, b * BS : (b + 1) * BS] = hot.astype(BF)
        qa[c, HD + 16 : 128] = jnp.zeros((128 - HD - 16, TOK), BF)

    seen = set()
    pending = []
    turn = [0]

    def scores(slot, c, n, buf):
        sc = jnp.dot(ka[slot, 0:n], qa[c], preferred_element_type=F32)
        buf[0:n] = sc
        buf[TOK : TOK + 8] = jnp.max(sc.reshape(n // 8, 8, TOK), axis=0)

    def soften(slot, c, n, buf):
        new = jnp.max(buf[TOK : TOK + 8], axis=0, keepdims=True)
        if c in seen:
            old = mx[c, 0:1]
            new = jnp.maximum(old, new)
            shrink = jnp.exp2((old - new) * RATE)
        pr = jnp.exp2((buf[0:n] - new) * RATE).astype(BF)
        upd = jnp.dot(va[slot, :, 0:n], pr, preferred_element_type=F32)
        if c in seen:
            acc[c] = acc[c] * shrink + upd
        else:
            acc[c] = upd
        mx[c, 0:1] = new
        seen.add(c)

    def flush():
        while pending:
            soften(*pending.pop(0))

    def steps(*pairs):
        for slot, c in pairs:
            n = tail if slot == ZL + TSLOTS - 1 else TOK
            buf = (s0, s1)[turn[0] % 2]
            turn[0] += 1
            scores(slot, c, n, buf)
            flush()
            pending.append((slot, c, n, buf))

    def origin_block(slot):
        return (((z + slot) % ZL) * YL + y) * (TOK // BS)

    o_cps = [None] * YL
    st_cps = [None] * YL

    def send_part(c):
        osend[c - 1] = acc[c, 0:HD].astype(BF)
        for a in range(4):
            ssend[c - 1, a : a + 1] = mx[c, 0:1, a * 128 : (a + 1) * 128]
            ssend[c - 1, 4 + a : 5 + a] = acc[c, HD : HD + 1, a * 128 : (a + 1) * 128]
        dev = {"blk": ypeer[c]}
        o_cps[c] = send(osend.at[c - 1], orecv.at[c - 1], o_s.at[c - 1], o_r.at[c - 1], dev)
        st_cps[c] = send(ssend.at[c - 1], srecv.at[c - 1], st_s.at[c - 1], st_r.at[c - 1], dev)

    ntext = tk_hbm.shape[1]
    edge = (TSLOTS - 1) * TOK
    tail = -(-(ntext - edge) // 128) * 128
    for cp in loads[:4]:
        cp.wait()
    with jax.named_scope("barrier"):
        pl.semaphore_wait(barrier, 5 + NH - 1)

    q_cps = [None] + [q_copy(c) for c in (1, 2, 3)]
    for kind in ("rk", "lk", "rv", "lv"):
        kv_send(kind, 1)
    loads[4].wait()
    for s in (4, 12, 8):
        w_copy(0, s)
    w_copy(0, 1)

    fill_queries(0)
    fill_keys(0, blk * (TOK // BS))
    loads[5].wait()
    loads[6].wait()
    for n, ref in ((0, tk_ref), (1, tv_ref)):
        tpad[n, :, edge:] = jnp.zeros((HD, TOK), BF)
        tpad[n, :, 0:ntext] = ref[...]
    for t in range(TSLOTS):
        row = iota((HD, TOK), 0)
        col = iota((HD, TOK), 1) + t * TOK
        inside = (col >= row * TEXT) & (col < (row + 1) * TEXT)
        gap = jnp.where((row < 8) & jnp.logical_not(inside), FAR, 0.0)
        span = slice(t * TOK, (t + 1) * TOK)
        wide = jnp.concatenate([tpad[0, :, span].astype(F32), gap], axis=0)
        ka[ZL + t] = wide.T.astype(BF)
        va[ZL + t, 0:HD] = tpad[1, :, span]
        va[ZL + t, HD : HD + 16] = jnp.ones((16, TOK), BF)

    with jax.named_scope("text"):
        steps((8, 0), (9, 0), (10, 0), (0, 0))
        flush()
    with jax.named_scope("qwait1"):
        q_cps[1].wait_recv()
    fill_queries(1)
    steps((0, 1))
    flush()
    with jax.named_scope("k1"):
        kv_hop("k", 1)
    with jax.named_scope("v1"):
        kv_hop("v", 1)
    w_copy(0, 2, 0)
    fill_keys(7, origin_block(7))
    fill_keys(1, origin_block(1))
    steps((7, 1), (1, 1), (7, 0))
    with jax.named_scope("k2"):
        kv_hop("k", 2)
    with jax.named_scope("qwait2"):
        q_cps[2].wait_recv()
    w_copy(0, 2, 1)
    fill_queries(2)
    steps((0, 2), (7, 2), (1, 2))
    with jax.named_scope("v2"):
        kv_hop("v", 2)
    fill_keys(6, origin_block(6))
    fill_keys(2, origin_block(2))
    steps((6, 1), (2, 1), (6, 2), (2, 2))
    with jax.named_scope("k3"):
        kv_hop("k", 3)
    with jax.named_scope("qwait3"):
        q_cps[3].wait_recv()
    fill_queries(3)
    steps((0, 3), (7, 3), (1, 3))
    with jax.named_scope("v3"):
        kv_hop("v", 3)
    fill_keys(5, origin_block(5))
    fill_keys(3, origin_block(3))
    steps((6, 3), (2, 3), (5, 3), (3, 3))
    with jax.named_scope("k4"):
        kv_hop("k", 4)
    steps((5, 2), (3, 2))
    with jax.named_scope("v4"):
        kv_hop("v", 4)
    fill_keys(4, origin_block(4))
    steps((4, 3), (4, 2))
    send_part(3)
    steps((5, 1))
    send_part(2)
    steps((3, 1), (4, 1))
    with jax.named_scope("wywait"):
        w_wait(2, 0)
    for s in (4, 12, 8):
        w_copy(2, s, 0)
    steps((1, 0))
    send_part(1)
    steps((6, 0), (2, 0))
    for s in (4, 12, 8):
        w_wait(s)
        w_copy(s, 1)
    steps((5, 0), (3, 0), (4, 0))
    flush()
    with jax.named_scope("wywait2"):
        w_wait(2, 1)
    for s in (4, 12, 8):
        w_copy(2, s, 1)
    w_copy(2, 1)
    with jax.named_scope("owait"):
        for c in (1, 2, 3):
            o_cps[c].wait_recv()
            st_cps[c].wait_recv()

    def row_of(ref, c, first):
        return jnp.concatenate([ref[c - 1, first + a : first + a + 1] for a in range(4)], axis=1)

    maxes = [mx[0, 0:1]] + [row_of(srecv, c, 0) for c in (1, 2, 3)]
    sums = [acc[0, HD : HD + 1]] + [row_of(srecv, c, 4) for c in (1, 2, 3)]
    top = functools.reduce(jnp.maximum, maxes)
    scales = [jnp.exp2((m - top) * RATE) for m in maxes]
    denom = functools.reduce(jnp.add, [s * l for s, l in zip(scales, sums)])
    numer = acc[0, 0:HD] * scales[0]
    for c in (1, 2, 3):
        numer = numer + orecv[c - 1].astype(F32) * scales[c]
    att = numer / denom
    both = jnp.concatenate([att, att], axis=0).T
    half = ROWS // 2
    side = iota((half, 128), 1) < HD
    for j in range(NH):
        one = both[j * ROWS : j * ROWS + half]
        two = both[j * ROWS + half : (j + 1) * ROWS]
        packed[j] = jnp.where(side, one, two).astype(BF)

    a_cps = []
    for s in (10, 11, 2, 3, 6, 7, 14, 15, 8, 9, 4, 5, 12, 13, 1):
        a_cps.append(
            send(packed.at[hpeer[s]], arecv.at[s - 1], a_s.at[s - 1], a_r.at[s - 1], {"head": hpeer[s]})
        )
    for s in (6, 14, 10):
        with jax.named_scope("wxwait2"):
            w_wait(s, 0)
            w_wait(s, 1)
        w_copy(s, 1)
    mine = packed[head].astype(F32)
    with jax.named_scope("await"):
        for cp in a_cps:
            cp.wait_recv()
    loads[7].wait()
    loads[8].wait()
    with jax.named_scope("wcwait"):
        for s in (1, 5, 13, 9, 3, 7, 15, 11):
            w_wait(s)
    pairs = []
    for i in range(NH // 2):
        even = mine if i == 0 else arecv[2 * i - 1].astype(F32)
        odd = arecv[2 * i].astype(F32)
        upper = jnp.where(side, even, pltpu.roll(odd, HD, 1))
        lower = jnp.where(side, pltpu.roll(even, HD, 1), odd)
        pairs.append(jnp.concatenate([upper, lower], axis=0).astype(BF))
    mixed = jnp.concatenate(pairs, axis=1)
    image = img_ref[blk * (TOK // BS) + head // (NH * BS // TOK)]
    gating = gate_ref[pl.ds(image, 1), :]
    projected = jnp.dot(mixed, wbuf[...], preferred_element_type=F32)
    out_ref[...] = (res_ref[...].astype(F32) + gating * projected).astype(BF)
    with jax.named_scope("sendwait"):
        for cp in started:
            cp.wait_send()


def on_device(queries, key_rows, values, text_keys, text_values, block_image, gate_image, residual, w_out):
    vm = pl.BlockSpec(memory_space=pltpu.VMEM)
    hb = pl.BlockSpec(memory_space=pl.ANY)
    dma = pltpu.SemaphoreType.DMA
    return pl.pallas_call(
        kernel,
        out_shape=jax.ShapeDtypeStruct((ROWS, D), BF),
        in_specs=[hb] * 9,
        out_specs=vm,
        scratch_shapes=[
            pltpu.SMEM(block_image.shape, jnp.int32),
            pltpu.VMEM((ZL, 2 * HD, TOK), BF),
            pltpu.VMEM((YL, HD, TOK), BF),
            pltpu.VMEM((HD, text_keys.shape[0]), BF),
            pltpu.VMEM((HD, text_keys.shape[0]), BF),
            pltpu.VMEM(gate_image.shape, F32),
            pltpu.VMEM((ROWS, D), BF),
            pltpu.VMEM((YL, 128, TOK), BF),
            pltpu.VMEM((ZL + TSLOTS, TOK, 128), BF),
            pltpu.VMEM((ZL + TSLOTS, HD + 16, TOK), BF),
            pltpu.VMEM((YL, HD + 16, TOK), F32),
            pltpu.VMEM((YL, 8, TOK), F32),
            pltpu.VMEM((2, HD, TSLOTS * TOK), BF),
            pltpu.VMEM((TOK + 8, TOK), F32),
            pltpu.VMEM((TOK + 8, TOK), F32),
            pltpu.VMEM((3, HD, TOK), BF),
            pltpu.VMEM((3, HD, TOK), BF),
            pltpu.VMEM((3, 8, 128), F32),
            pltpu.VMEM((3, 8, 128), F32),
            pltpu.VMEM((NH, ROWS // 2, 128), BF),
            pltpu.VMEM((NH - 1, ROWS // 2, 128), BF),
            pltpu.VMEM((NH * HD, D), BF),
            dma((3,)), dma((3,)),
            dma((14,)), dma((14,)),
            dma((19,)), dma((32,)),
            dma((3,)), dma((3,)),
            dma((3,)), dma((3,)),
            dma((15,)), dma((15,)),
            dma((9,)),
        ],
        compiler_params=pltpu.CompilerParams(
            collective_id=0, has_side_effects=True, vmem_limit_bytes=60 * 1024 * 1024
        ),
        name="joint_attention",
    )(
        queries.T, key_rows.T, values.T, text_keys.T, text_values.T,
        block_image, gate_image, residual, w_out,
    )


def solution(mesh):
    placed = (
        P("blk", "head"),
        P("blk", "head"),
        P("blk", "head"),
        P(None, "head"),
        P(None, "head"),
        P(),
        P(),
        P(("blk", "head"), None),
        P("head", None),
    )
    return jax.shard_map(
        on_device, mesh=mesh, in_specs=placed, out_specs=P(("blk", "head"), None), check_vma=False
    )
```

```python
import functools
import math

import jax
import jax.numpy as jnp
from jax import lax
from jax.experimental import pallas as pl
from jax.experimental.pallas import tpu as pltpu
from jax.sharding import PartitionSpec as P

HD = 64
TEXT = 154
BS = 128
TOK = 512
YL = 4
ZL = 8
NH = 16
D = 1536
ROWS = TOK // NH
TSLOTS = 3
FAR = -(2.0**100)
RATE = math.log2(math.e) / math.sqrt(HD)
MESH = pl.DeviceIdType.MESH
BF = jnp.bfloat16
F32 = jnp.float32
NT = (((1,), (1,)), ((), ()))


def flip(index, mask, bits):
    total = 0
    for b in range(bits):
        bit = (index // (1 << b)) % 2
        total = total + (1 << b) * ((1 - bit) if (mask >> b) & 1 else bit)
    return total


def iota(shape, dim):
    return lax.broadcasted_iota(jnp.int32, shape, dim)


def kernel(
    q_hbm, k_hbm, v_hbm, tk_hbm, tv_hbm, img_hbm, gate_hbm, res_hbm, w_hbm,
    out_ref,
    img_ref, kv, qt, tk_ref, tv_ref, gate_ref, res_ref, qa, ka, va, acc, mx, tpad, s0, s1, osend, orecv, ssend, srecv, packed, arecv, wbuf,
    q_s, q_r, kv_s, kv_r, w_s, w_r, o_s, o_r, st_s, st_r, a_s, a_r, in_s, token,
):
    blk = lax.axis_index("blk")
    head = lax.axis_index("head")
    z = blk // YL
    y = blk % YL
    zright = ((z + 1) % ZL) * YL + y
    zleft = ((z + ZL - 1) % ZL) * YL + y
    ypeer = [z * YL + flip(y, c, 2) for c in range(YL)]
    hpeer = [flip(head, s, 4) for s in range(NH)]

    barrier = pltpu.get_barrier_semaphore()
    for other in (zright, zleft, ypeer[1], ypeer[2], ypeer[3]):
        pl.semaphore_signal(barrier, inc=1, device_id={"blk": other}, device_id_type=MESH)
    for s in (4, 12, 8, 2, 1):
        pl.semaphore_signal(barrier, inc=1, device_id={"head": hpeer[s]}, device_id_type=MESH)

    loads = [
        pltpu.make_async_copy(src, dst, in_s.at[n])
        for n, (src, dst) in enumerate((
            (img_hbm, img_ref),
            (q_hbm, qt.at[0]),
            (k_hbm, kv.at[0, pl.ds(0, HD)]),
            (v_hbm, kv.at[0, pl.ds(HD, HD)]),
            (w_hbm, wbuf.at[pl.ds(0, HD)]),
            (tk_hbm, tk_ref),
            (tv_hbm, tv_ref),
            (gate_hbm, gate_ref),
            (res_hbm, res_ref),
        ))
    ]
    for cp in loads:
        cp.start()

    started = []

    def send(src, dst, ssem, rsem, dev):
        copy = pltpu.make_async_remote_copy(
            src_ref=src, dst_ref=dst, send_sem=ssem, recv_sem=rsem,
            device_id=dev, device_id_type=MESH,
        )
        copy.start()
        started.append(copy)
        return copy

    def q_copy(c):
        return send(qt.at[0], qt.at[c], q_s.at[c - 1], q_r.at[c - 1], {"blk": ypeer[c]})

    kv_cps = {}

    def kv_send(kind, step, half):
        src = step - 1 if kind in ("lk", "lv") or step == 1 else ZL - (step - 1)
        dst = step if kind in ("lk", "lv") else ZL - step
        k = 2 * ({"rk": 0, "rv": 4, "lk": 7, "lv": 10}[kind] + step - 1) + half
        rows = pl.ds((0 if kind in ("rk", "lk") else HD) + half * (HD // 2), HD // 2)
        dev = {"blk": zleft if kind in ("lk", "lv") else zright}
        kv_cps[kind, step, half] = send(kv.at[src, rows], kv.at[dst, rows], kv_s.at[k], kv_r.at[k], dev)

    def kv_hop(part, step):
        for half in range(2):
            for kind in ("r" + part, "l" + part):
                if (kind, step, half) in kv_cps:
                    kv_cps[kind, step, half].wait_recv()
                    if step < {"rk": 4, "lk": 3, "rv": 3, "lv": 4}[kind]:
                        kv_send(kind, step + 1, half)

    w_count = [0]

    def w_part(slot, half):
        if half is None:
            return wbuf.at[pl.ds(slot * HD, HD)]
        return wbuf.at[pl.ds(slot * HD + half * (HD // 2), HD // 2)]

    def w_sem(slot, half):
        return w_r.at[slot if half in (None, 0) else NH + slot]

    def w_copy(origin, to, half=None):
        slot = origin ^ to
        k = w_count[0]
        w_count[0] += 1
        return send(w_part(origin, half), w_part(slot, half), w_s.at[k], w_sem(slot, half), {"head": hpeer[to]})

    def w_wait(slot, half=None):
        part = w_part(slot, half)
        pltpu.make_async_remote_copy(
            src_ref=part, dst_ref=part, send_sem=w_s.at[0], recv_sem=w_sem(slot, half),
            device_id={"head": hpeer[1]}, device_id_type=MESH,
        ).wait_recv()

    def fill_keys(slot, first_block):
        row = iota((HD, BS), 0)
        gaps = []
        for b in range(TOK // BS):
            image = img_ref[first_block + b]
            gaps.append(jnp.where((row < 8) & (row != image), FAR, 0.0))
        wide = jnp.concatenate([kv[slot, 0:HD].astype(F32), jnp.concatenate(gaps, axis=1)], axis=0)
        ka[slot] = wide.T.astype(BF)
        va[slot, 0:HD] = kv[slot, HD : 2 * HD]
        va[slot, HD : HD + 16] = jnp.ones((16, TOK), BF)

    def fill_queries(c):
        qa[c, 0:HD] = qt[c]
        first = ypeer[c] * (TOK // BS)
        for b in range(TOK // BS):
            image = img_ref[first + b]
            hot = (iota((16, BS), 0) == image).astype(F32)
            qa[c, HD : HD + 16, b * BS : (b + 1) * BS] = hot.astype(BF)
        qa[c, HD + 16 : 128] = jnp.zeros((128 - HD - 16, TOK), BF)

    seen = set()
    pending = []
    turn = [0]

    def scores(slot, c, n, buf):
        sc = jnp.dot(ka[slot, 0:n], qa[c], preferred_element_type=F32)
        buf[0:n] = sc
        buf[TOK : TOK + 8] = jnp.max(sc.reshape(n // 8, 8, TOK), axis=0)

    def soften(slot, c, n, buf):
        new = jnp.max(buf[TOK : TOK + 8], axis=0, keepdims=True)
        if c in seen:
            old = mx[c, 0:1]
            new = jnp.maximum(old, new)
            shrink = jnp.exp2((old - new) * RATE)
        pr = jnp.exp2((buf[0:n] - new) * RATE).astype(BF)
        upd = jnp.dot(va[slot, :, 0:n], pr, preferred_element_type=F32)
        if c in seen:
            acc[c] = acc[c] * shrink + upd
        else:
            acc[c] = upd
        mx[c, 0:1] = new
        seen.add(c)

    def flush():
        while pending:
            soften(*pending.pop(0))

    def steps(*pairs):
        for slot, c in pairs:
            n = tail if slot == ZL + TSLOTS - 1 else TOK
            buf = (s0, s1)[turn[0] % 2]
            turn[0] += 1
            scores(slot, c, n, buf)
            flush()
            pending.append((slot, c, n, buf))

    def origin_block(slot):
        return (((z + slot) % ZL) * YL + y) * (TOK // BS)

    o_cps = [None] * YL
    st_cps = [None] * YL

    def send_part(c):
        osend[c - 1] = acc[c, 0:HD].astype(BF)
        for a in range(4):
            ssend[c - 1, a : a + 1] = mx[c, 0:1, a * 128 : (a + 1) * 128]
            ssend[c - 1, 4 + a : 5 + a] = acc[c, HD : HD + 1, a * 128 : (a + 1) * 128]
        dev = {"blk": ypeer[c]}
        o_cps[c] = send(osend.at[c - 1], orecv.at[c - 1], o_s.at[c - 1], o_r.at[c - 1], dev)
        st_cps[c] = send(ssend.at[c - 1], srecv.at[c - 1], st_s.at[c - 1], st_r.at[c - 1], dev)

    ntext = tk_hbm.shape[1]
    edge = (TSLOTS - 1) * TOK
    tail = -(-(ntext - edge) // 128) * 128
    for cp in loads[:4]:
        cp.wait()
    with jax.named_scope("barrier"):
        pl.semaphore_wait(barrier, 10)

    q_cps = [None] + [q_copy(c) for c in (1, 2, 3)]
    for part in ("k", "v"):
        for half in range(2):
            kv_send("r" + part, 1, half)
            kv_send("l" + part, 1, half)
    pl.semaphore_signal(token.at[0], inc=1, device_id={"head": hpeer[2]}, device_id_type=MESH)
    loads[4].wait()
    for s in (4, 12, 8):
        w_copy(0, s)
    w_copy(0, 1)

    fill_queries(0)
    fill_keys(0, blk * (TOK // BS))
    loads[5].wait()
    loads[6].wait()
    for n, ref in ((0, tk_ref), (1, tv_ref)):
        tpad[n, :, edge:] = jnp.zeros((HD, TOK), BF)
        tpad[n, :, 0:ntext] = ref[...]
    for t in range(TSLOTS):
        row = iota((HD, TOK), 0)
        col = iota((HD, TOK), 1) + t * TOK
        inside = (col >= row * TEXT) & (col < (row + 1) * TEXT)
        gap = jnp.where((row < 8) & jnp.logical_not(inside), FAR, 0.0)
        span = slice(t * TOK, (t + 1) * TOK)
        wide = jnp.concatenate([tpad[0, :, span].astype(F32), gap], axis=0)
        ka[ZL + t] = wide.T.astype(BF)
        va[ZL + t, 0:HD] = tpad[1, :, span]
        va[ZL + t, HD : HD + 16] = jnp.ones((16, TOK), BF)

    with jax.named_scope("text"):
        steps((8, 0), (9, 0), (10, 0), (0, 0))
        flush()
    w_copy(0, 2, 0)
    with jax.named_scope("qwait1"):
        q_cps[1].wait_recv()
    fill_queries(1)
    steps((0, 1))
    flush()
    with jax.named_scope("k1"):
        kv_hop("k", 1)
    with jax.named_scope("v1"):
        kv_hop("v", 1)
    w_copy(0, 2, 1)
    pl.semaphore_wait(token.at[0], 1)
    pl.semaphore_signal(token.at[1], inc=1, device_id={"head": hpeer[1]}, device_id_type=MESH)
    fill_keys(7, origin_block(7))
    fill_keys(1, origin_block(1))
    steps((7, 1), (1, 1), (7, 0), (1, 0))
    with jax.named_scope("k2"):
        kv_hop("k", 2)
    with jax.named_scope("qwait2"):
        q_cps[2].wait_recv()
    fill_queries(2)
    steps((0, 2), (7, 2), (1, 2))
    with jax.named_scope("v2"):
        kv_hop("v", 2)
    fill_keys(6, origin_block(6))
    fill_keys(2, origin_block(2))
    steps((6, 1), (2, 1), (6, 2), (2, 2))
    with jax.named_scope("k3"):
        kv_hop("k", 3)
    with jax.named_scope("qwait3"):
        q_cps[3].wait_recv()
    fill_queries(3)
    steps((0, 3), (7, 3), (1, 3))
    with jax.named_scope("v3"):
        kv_hop("v", 3)
    fill_keys(5, origin_block(5))
    fill_keys(3, origin_block(3))
    steps((6, 3), (2, 3), (5, 3), (3, 3))
    with jax.named_scope("wywait"):
        w_wait(2, 0)
    for s in (4, 12, 8):
        w_copy(2, s, 0)
    with jax.named_scope("k4"):
        kv_hop("k", 4)
    steps((5, 2), (3, 2), (5, 1))
    with jax.named_scope("v4"):
        kv_hop("v", 4)
    fill_keys(4, origin_block(4))
    steps((4, 3), (4, 2))
    send_part(3)
    steps((3, 1))
    send_part(2)
    with jax.named_scope("wywait2"):
        w_wait(2, 1)
    for s in (4, 12, 8):
        w_copy(2, s, 1)
    w_copy(2, 1)
    steps((4, 1), (6, 0))
    send_part(1)
    for s in (4, 12, 8):
        w_wait(s)
        w_copy(s, 1)
    steps((2, 0), (5, 0), (3, 0), (4, 0))
    flush()
    pl.semaphore_wait(token.at[1], 1)
    with jax.named_scope("owait"):
        for c in (1, 2, 3):
            o_cps[c].wait_recv()
            st_cps[c].wait_recv()

    def row_of(ref, c, first):
        return jnp.concatenate([ref[c - 1, first + a : first + a + 1] for a in range(4)], axis=1)

    maxes = [mx[0, 0:1]] + [row_of(srecv, c, 0) for c in (1, 2, 3)]
    sums = [acc[0, HD : HD + 1]] + [row_of(srecv, c, 4) for c in (1, 2, 3)]
    top = functools.reduce(jnp.maximum, maxes)
    scales = [jnp.exp2((m - top) * RATE) for m in maxes]
    denom = functools.reduce(jnp.add, [s * l for s, l in zip(scales, sums)])
    numer = acc[0, 0:HD] * scales[0]
    for c in (1, 2, 3):
        numer = numer + orecv[c - 1].astype(F32) * scales[c]
    att = numer / denom
    both = jnp.concatenate([att, att], axis=0).T
    half = ROWS // 2
    side = iota((half, 128), 1) < HD
    for j in range(NH):
        one = both[j * ROWS : j * ROWS + half]
        two = both[j * ROWS + half : (j + 1) * ROWS]
        packed[j] = jnp.where(side, one, two).astype(BF)

    a_cps = []
    for s in (10, 11, 2, 3, 6, 7, 14, 15, 8, 9, 4, 5, 12, 13, 1):
        a_cps.append(
            send(packed.at[hpeer[s]], arecv.at[s - 1], a_s.at[s - 1], a_r.at[s - 1], {"head": hpeer[s]})
        )
    for s in (6, 14, 10):
        with jax.named_scope("wxwait2"):
            w_wait(s, 0)
            w_wait(s, 1)
        w_copy(s, 1)
    mine = packed[head].astype(F32)
    with jax.named_scope("await"):
        for cp in a_cps:
            cp.wait_recv()
    loads[7].wait()
    loads[8].wait()
    with jax.named_scope("wcwait"):
        for s in (1, 5, 13, 9, 3, 7, 15, 11):
            w_wait(s)
    pairs = []
    for i in range(NH // 2):
        even = mine if i == 0 else arecv[2 * i - 1].astype(F32)
        odd = arecv[2 * i].astype(F32)
        upper = jnp.where(side, even, pltpu.roll(odd, HD, 1))
        lower = jnp.where(side, pltpu.roll(even, HD, 1), odd)
        pairs.append(jnp.concatenate([upper, lower], axis=0).astype(BF))
    mixed = jnp.concatenate(pairs, axis=1)
    image = img_ref[blk * (TOK // BS) + head // (NH * BS // TOK)]
    gating = gate_ref[pl.ds(image, 1), :]
    projected = jnp.dot(mixed, wbuf[...], preferred_element_type=F32)
    out_ref[...] = (res_ref[...].astype(F32) + gating * projected).astype(BF)
    with jax.named_scope("sendwait"):
        for cp in started:
            cp.wait_send()


def on_device(queries, key_rows, values, text_keys, text_values, block_image, gate_image, residual, w_out):
    vm = pl.BlockSpec(memory_space=pltpu.VMEM)
    hb = pl.BlockSpec(memory_space=pl.ANY)
    dma = pltpu.SemaphoreType.DMA
    return pl.pallas_call(
        kernel,
        out_shape=jax.ShapeDtypeStruct((ROWS, D), BF),
        in_specs=[hb] * 9,
        out_specs=vm,
        scratch_shapes=[
            pltpu.SMEM(block_image.shape, jnp.int32),
            pltpu.VMEM((ZL, 2 * HD, TOK), BF),
            pltpu.VMEM((YL, HD, TOK), BF),
            pltpu.VMEM((HD, text_keys.shape[0]), BF),
            pltpu.VMEM((HD, text_keys.shape[0]), BF),
            pltpu.VMEM(gate_image.shape, F32),
            pltpu.VMEM((ROWS, D), BF),
            pltpu.VMEM((YL, 128, TOK), BF),
            pltpu.VMEM((ZL + TSLOTS, TOK, 128), BF),
            pltpu.VMEM((ZL + TSLOTS, HD + 16, TOK), BF),
            pltpu.VMEM((YL, HD + 16, TOK), F32),
            pltpu.VMEM((YL, 8, TOK), F32),
            pltpu.VMEM((2, HD, TSLOTS * TOK), BF),
            pltpu.VMEM((TOK + 8, TOK), F32),
            pltpu.VMEM((TOK + 8, TOK), F32),
            pltpu.VMEM((3, HD, TOK), BF),
            pltpu.VMEM((3, HD, TOK), BF),
            pltpu.VMEM((3, 8, 128), F32),
            pltpu.VMEM((3, 8, 128), F32),
            pltpu.VMEM((NH, ROWS // 2, 128), BF),
            pltpu.VMEM((NH - 1, ROWS // 2, 128), BF),
            pltpu.VMEM((NH * HD, D), BF),
            dma((3,)), dma((3,)),
            dma((28,)), dma((28,)),
            dma((19,)), dma((32,)),
            dma((3,)), dma((3,)),
            dma((3,)), dma((3,)),
            dma((15,)), dma((15,)),
            dma((9,)),
            pltpu.SemaphoreType.REGULAR((2,)),
        ],
        compiler_params=pltpu.CompilerParams(
            collective_id=0, has_side_effects=True, vmem_limit_bytes=60 * 1024 * 1024
        ),
        name="joint_attention",
    )(
        queries.T, key_rows.T, values.T, text_keys.T, text_values.T,
        block_image, gate_image, residual, w_out,
    )


def solution(mesh):
    placed = (
        P("blk", "head"),
        P("blk", "head"),
        P("blk", "head"),
        P(None, "head"),
        P(None, "head"),
        P(),
        P(),
        P(("blk", "head"), None),
        P("head", None),
    )
    return jax.shard_map(
        on_device, mesh=mesh, in_specs=placed, out_specs=P(("blk", "head"), None), check_vma=False
    )
```

```python
import functools
import math

import jax
import jax.numpy as jnp
from jax import lax
from jax.experimental import pallas as pl
from jax.experimental.pallas import tpu as pltpu
from jax.sharding import PartitionSpec as P

HD = 64
TEXT = 154
BS = 128
TOK = 512
YL = 4
ZL = 8
NH = 16
D = 1536
ROWS = TOK // NH
TSLOTS = 3
FAR = -(2.0**100)
RATE = math.log2(math.e) / math.sqrt(HD)
MESH = pl.DeviceIdType.MESH
BF = jnp.bfloat16
F32 = jnp.float32
NT = (((1,), (1,)), ((), ()))


def flip(index, mask, bits):
    total = 0
    for b in range(bits):
        bit = (index // (1 << b)) % 2
        total = total + (1 << b) * ((1 - bit) if (mask >> b) & 1 else bit)
    return total


def iota(shape, dim):
    return lax.broadcasted_iota(jnp.int32, shape, dim)


def kernel(
    q_hbm, k_hbm, v_hbm, tk_hbm, tv_hbm, img_hbm, gate_hbm, res_hbm, w_hbm,
    out_ref,
    img_ref, kv, qt, tk_ref, tv_ref, gate_ref, res_ref, qa, ka, va, acc, mx, tpad, s0, s1, osend, orecv, ssend, srecv, packed, arecv, wbuf,
    q_s, q_r, kv_s, kv_r, w_s, w_r, o_s, o_r, st_s, st_r, a_s, a_r, in_s, token,
):
    blk = lax.axis_index("blk")
    head = lax.axis_index("head")
    z = blk // YL
    y = blk % YL
    zright = ((z + 1) % ZL) * YL + y
    zleft = ((z + ZL - 1) % ZL) * YL + y
    ypeer = [z * YL + flip(y, c, 2) for c in range(YL)]
    hpeer = [flip(head, s, 4) for s in range(NH)]

    barrier = pltpu.get_barrier_semaphore()
    for other in (zright, zleft, ypeer[1], ypeer[2], ypeer[3]):
        pl.semaphore_signal(barrier, inc=1, device_id={"blk": other}, device_id_type=MESH)
    for s in (4, 12, 8, 2, 1):
        pl.semaphore_signal(barrier, inc=1, device_id={"head": hpeer[s]}, device_id_type=MESH)

    loads = [
        pltpu.make_async_copy(src, dst, in_s.at[n])
        for n, (src, dst) in enumerate((
            (img_hbm, img_ref),
            (q_hbm, qt.at[0]),
            (k_hbm, kv.at[0, pl.ds(0, HD)]),
            (v_hbm, kv.at[0, pl.ds(HD, HD)]),
            (w_hbm, wbuf.at[pl.ds(0, HD)]),
            (tk_hbm, tk_ref),
            (tv_hbm, tv_ref),
            (gate_hbm, gate_ref),
            (res_hbm, res_ref),
        ))
    ]
    for cp in loads:
        cp.start()

    started = []

    def send(src, dst, ssem, rsem, dev):
        copy = pltpu.make_async_remote_copy(
            src_ref=src, dst_ref=dst, send_sem=ssem, recv_sem=rsem,
            device_id=dev, device_id_type=MESH,
        )
        copy.start()
        started.append(copy)
        return copy

    def q_copy(c):
        return send(qt.at[0], qt.at[c], q_s.at[c - 1], q_r.at[c - 1], {"blk": ypeer[c]})

    kv_cps = {}

    def kv_send(kind, step, half):
        src = step - 1 if kind in ("lk", "lv") or step == 1 else ZL - (step - 1)
        dst = step if kind in ("lk", "lv") else ZL - step
        k = 2 * ({"rk": 0, "rv": 4, "lk": 7, "lv": 10}[kind] + step - 1) + half
        rows = pl.ds((0 if kind in ("rk", "lk") else HD) + half * (HD // 2), HD // 2)
        dev = {"blk": zleft if kind in ("lk", "lv") else zright}
        kv_cps[kind, step, half] = send(kv.at[src, rows], kv.at[dst, rows], kv_s.at[k], kv_r.at[k], dev)

    def kv_hop(part, step):
        for half in range(2):
            for kind in ("r" + part, "l" + part):
                if (kind, step, half) in kv_cps:
                    kv_cps[kind, step, half].wait_recv()
                    if step < {"rk": 4, "lk": 3, "rv": 3, "lv": 4}[kind]:
                        kv_send(kind, step + 1, half)

    w_count = [0]

    def w_part(slot, half):
        if half is None:
            return wbuf.at[pl.ds(slot * HD, HD)]
        return wbuf.at[pl.ds(slot * HD + half * (HD // 2), HD // 2)]

    def w_sem(slot, half):
        return w_r.at[slot if half in (None, 0) else NH + slot]

    def w_copy(origin, to, half=None):
        slot = origin ^ to
        k = w_count[0]
        w_count[0] += 1
        return send(w_part(origin, half), w_part(slot, half), w_s.at[k], w_sem(slot, half), {"head": hpeer[to]})

    def w_wait(slot, half=None):
        part = w_part(slot, half)
        pltpu.make_async_remote_copy(
            src_ref=part, dst_ref=part, send_sem=w_s.at[0], recv_sem=w_sem(slot, half),
            device_id={"head": hpeer[1]}, device_id_type=MESH,
        ).wait_recv()

    def fill_keys(slot, first_block):
        row = iota((HD, BS), 0)
        gaps = []
        for b in range(TOK // BS):
            image = img_ref[first_block + b]
            gaps.append(jnp.where((row < 8) & (row != image), FAR, 0.0))
        wide = jnp.concatenate([kv[slot, 0:HD].astype(F32), jnp.concatenate(gaps, axis=1)], axis=0)
        ka[slot] = wide.T.astype(BF)
        va[slot, 0:HD] = kv[slot, HD : 2 * HD]
        va[slot, HD : HD + 16] = jnp.ones((16, TOK), BF)

    def fill_queries(c):
        qa[c, 0:HD] = qt[c]
        first = ypeer[c] * (TOK // BS)
        for b in range(TOK // BS):
            image = img_ref[first + b]
            hot = (iota((16, BS), 0) == image).astype(F32)
            qa[c, HD : HD + 16, b * BS : (b + 1) * BS] = hot.astype(BF)
        qa[c, HD + 16 : 128] = jnp.zeros((128 - HD - 16, TOK), BF)

    seen = set()
    pending = []
    turn = [0]

    def scores(slot, c, n, buf):
        sc = jnp.dot(ka[slot, 0:n], qa[c], preferred_element_type=F32)
        buf[0:n] = sc
        buf[TOK : TOK + 8] = jnp.max(sc.reshape(n // 8, 8, TOK), axis=0)

    def soften(slot, c, n, buf):
        new = jnp.max(buf[TOK : TOK + 8], axis=0, keepdims=True)
        if c in seen:
            old = mx[c, 0:1]
            new = jnp.maximum(old, new)
            shrink = jnp.exp2((old - new) * RATE)
        pr = jnp.exp2((buf[0:n] - new) * RATE).astype(BF)
        upd = jnp.dot(va[slot, :, 0:n], pr, preferred_element_type=F32)
        if c in seen:
            acc[c] = acc[c] * shrink + upd
        else:
            acc[c] = upd
        mx[c, 0:1] = new
        seen.add(c)

    def flush():
        while pending:
            soften(*pending.pop(0))

    def steps(*pairs):
        for slot, c in pairs:
            n = tail if slot == ZL + TSLOTS - 1 else TOK
            buf = (s0, s1)[turn[0] % 2]
            turn[0] += 1
            scores(slot, c, n, buf)
            flush()
            pending.append((slot, c, n, buf))

    def origin_block(slot):
        return (((z + slot) % ZL) * YL + y) * (TOK // BS)

    o_cps = [None] * YL
    st_cps = [None] * YL

    def send_part(c):
        osend[c - 1] = acc[c, 0:HD].astype(BF)
        for a in range(4):
            ssend[c - 1, a : a + 1] = mx[c, 0:1, a * 128 : (a + 1) * 128]
            ssend[c - 1, 4 + a : 5 + a] = acc[c, HD : HD + 1, a * 128 : (a + 1) * 128]
        dev = {"blk": ypeer[c]}
        o_cps[c] = send(osend.at[c - 1], orecv.at[c - 1], o_s.at[c - 1], o_r.at[c - 1], dev)
        st_cps[c] = send(ssend.at[c - 1], srecv.at[c - 1], st_s.at[c - 1], st_r.at[c - 1], dev)

    ntext = tk_hbm.shape[1]
    edge = (TSLOTS - 1) * TOK
    tail = -(-(ntext - edge) // 128) * 128
    for cp in loads[:4]:
        cp.wait()
    with jax.named_scope("barrier"):
        pl.semaphore_wait(barrier, 10)

    q_cps = [None] + [q_copy(c) for c in (1, 2, 3)]
    for part in ("k", "v"):
        for half in range(2):
            kv_send("r" + part, 1, half)
            kv_send("l" + part, 1, half)
    pl.semaphore_signal(token.at[0], inc=1, device_id={"head": hpeer[2]}, device_id_type=MESH)
    loads[4].wait()
    for s in (4, 12, 8):
        w_copy(0, s)
    w_copy(0, 1)

    fill_queries(0)
    fill_keys(0, blk * (TOK // BS))
    loads[5].wait()
    loads[6].wait()
    for n, ref in ((0, tk_ref), (1, tv_ref)):
        tpad[n, :, edge:] = jnp.zeros((HD, TOK), BF)
        tpad[n, :, 0:ntext] = ref[...]
    for t in range(TSLOTS):
        row = iota((HD, TOK), 0)
        col = iota((HD, TOK), 1) + t * TOK
        inside = (col >= row * TEXT) & (col < (row + 1) * TEXT)
        gap = jnp.where((row < 8) & jnp.logical_not(inside), FAR, 0.0)
        span = slice(t * TOK, (t + 1) * TOK)
        wide = jnp.concatenate([tpad[0, :, span].astype(F32), gap], axis=0)
        ka[ZL + t] = wide.T.astype(BF)
        va[ZL + t, 0:HD] = tpad[1, :, span]
        va[ZL + t, HD : HD + 16] = jnp.ones((16, TOK), BF)

    with jax.named_scope("text"):
        steps((8, 0), (9, 0), (10, 0), (0, 0))
        flush()
    with jax.named_scope("k1"):
        kv_hop("k", 1)
    with jax.named_scope("v1"):
        kv_hop("v", 1)
    fill_keys(7, origin_block(7))
    fill_keys(1, origin_block(1))
    steps((7, 0), (1, 0))
    with jax.named_scope("qwait1"):
        q_cps[1].wait_recv()
    w_copy(0, 2, 0)
    pl.semaphore_wait(token.at[0], 1)
    pl.semaphore_signal(token.at[1], inc=1, device_id={"head": hpeer[1]}, device_id_type=MESH)
    fill_queries(1)
    steps((0, 1), (7, 1), (1, 1))
    with jax.named_scope("k2"):
        kv_hop("k", 2)
    with jax.named_scope("qwait2"):
        q_cps[2].wait_recv()
    w_copy(0, 2, 1)
    fill_queries(2)
    steps((0, 2), (7, 2), (1, 2))
    with jax.named_scope("v2"):
        kv_hop("v", 2)
    fill_keys(6, origin_block(6))
    fill_keys(2, origin_block(2))
    steps((6, 1), (2, 1), (6, 2), (2, 2))
    with jax.named_scope("k3"):
        kv_hop("k", 3)
    steps((6, 0), (2, 0))
    with jax.named_scope("v3"):
        kv_hop("v", 3)
    fill_keys(5, origin_block(5))
    fill_keys(3, origin_block(3))
    steps((5, 1), (3, 1))
    with jax.named_scope("qwait3"):
        q_cps[3].wait_recv()
    fill_queries(3)
    steps((0, 3), (7, 3))
    with jax.named_scope("k4"):
        kv_hop("k", 4)
    for s in (4, 12, 8):
        w_wait(s)
        w_copy(s, 1)
    steps((1, 3), (6, 3), (2, 3))
    with jax.named_scope("v4"):
        kv_hop("v", 4)
    fill_keys(4, origin_block(4))
    steps((5, 3), (3, 3))
    with jax.named_scope("wywait"):
        w_wait(2, 0)
    for s in (4, 12, 8):
        w_copy(2, s, 0)
    steps((4, 3), (5, 2))
    send_part(3)
    steps((3, 2), (4, 2), (4, 1))
    send_part(2)
    with jax.named_scope("wywait2"):
        w_wait(2, 1)
    for s in (4, 12, 8):
        w_copy(2, s, 1)
    w_copy(2, 1)
    steps((5, 0))
    send_part(1)
    steps((3, 0), (4, 0))
    flush()
    pl.semaphore_wait(token.at[1], 1)
    with jax.named_scope("owait"):
        for c in (1, 2, 3):
            o_cps[c].wait_recv()
            st_cps[c].wait_recv()

    def row_of(ref, c, first):
        return jnp.concatenate([ref[c - 1, first + a : first + a + 1] for a in range(4)], axis=1)

    maxes = [mx[0, 0:1]] + [row_of(srecv, c, 0) for c in (1, 2, 3)]
    sums = [acc[0, HD : HD + 1]] + [row_of(srecv, c, 4) for c in (1, 2, 3)]
    top = functools.reduce(jnp.maximum, maxes)
    scales = [jnp.exp2((m - top) * RATE) for m in maxes]
    denom = functools.reduce(jnp.add, [s * l for s, l in zip(scales, sums)])
    numer = acc[0, 0:HD] * scales[0]
    for c in (1, 2, 3):
        numer = numer + orecv[c - 1].astype(F32) * scales[c]
    att = numer / denom
    both = jnp.concatenate([att, att], axis=0).T
    half = ROWS // 2
    side = iota((half, 128), 1) < HD
    for j in range(NH):
        one = both[j * ROWS : j * ROWS + half]
        two = both[j * ROWS + half : (j + 1) * ROWS]
        packed[j] = jnp.where(side, one, two).astype(BF)

    a_cps = []
    for s in (10, 11, 2, 3, 6, 7, 14, 15, 8, 9, 4, 5, 12, 13, 1):
        a_cps.append(
            send(packed.at[hpeer[s]], arecv.at[s - 1], a_s.at[s - 1], a_r.at[s - 1], {"head": hpeer[s]})
        )
    for s in (6, 14, 10):
        with jax.named_scope("wxwait2"):
            w_wait(s, 0)
            w_wait(s, 1)
        w_copy(s, 1)
    mine = packed[head].astype(F32)
    with jax.named_scope("await"):
        for cp in a_cps:
            cp.wait_recv()
    loads[7].wait()
    loads[8].wait()
    with jax.named_scope("wcwait"):
        for s in (1, 5, 13, 9, 3, 7, 15, 11):
            w_wait(s)
    pairs = []
    for i in range(NH // 2):
        even = mine if i == 0 else arecv[2 * i - 1].astype(F32)
        odd = arecv[2 * i].astype(F32)
        upper = jnp.where(side, even, pltpu.roll(odd, HD, 1))
        lower = jnp.where(side, pltpu.roll(even, HD, 1), odd)
        pairs.append(jnp.concatenate([upper, lower], axis=0).astype(BF))
    mixed = jnp.concatenate(pairs, axis=1)
    image = img_ref[blk * (TOK // BS) + head // (NH * BS // TOK)]
    gating = gate_ref[pl.ds(image, 1), :]
    projected = jnp.dot(mixed, wbuf[...], preferred_element_type=F32)
    out_ref[...] = (res_ref[...].astype(F32) + gating * projected).astype(BF)
    with jax.named_scope("sendwait"):
        for cp in started:
            cp.wait_send()


def on_device(queries, key_rows, values, text_keys, text_values, block_image, gate_image, residual, w_out):
    vm = pl.BlockSpec(memory_space=pltpu.VMEM)
    hb = pl.BlockSpec(memory_space=pl.ANY)
    dma = pltpu.SemaphoreType.DMA
    return pl.pallas_call(
        kernel,
        out_shape=pltpu.VMEM((ROWS, D), BF),
        in_specs=[hb] * 9,
        out_specs=vm,
        scratch_shapes=[
            pltpu.SMEM(block_image.shape, jnp.int32),
            pltpu.VMEM((ZL, 2 * HD, TOK), BF),
            pltpu.VMEM((YL, HD, TOK), BF),
            pltpu.VMEM((HD, text_keys.shape[0]), BF),
            pltpu.VMEM((HD, text_keys.shape[0]), BF),
            pltpu.VMEM(gate_image.shape, F32),
            pltpu.VMEM((ROWS, D), BF),
            pltpu.VMEM((YL, 128, TOK), BF),
            pltpu.VMEM((ZL + TSLOTS, TOK, 128), BF),
            pltpu.VMEM((ZL + TSLOTS, HD + 16, TOK), BF),
            pltpu.VMEM((YL, HD + 16, TOK), F32),
            pltpu.VMEM((YL, 8, TOK), F32),
            pltpu.VMEM((2, HD, TSLOTS * TOK), BF),
            pltpu.VMEM((TOK + 8, TOK), F32),
            pltpu.VMEM((TOK + 8, TOK), F32),
            pltpu.VMEM((3, HD, TOK), BF),
            pltpu.VMEM((3, HD, TOK), BF),
            pltpu.VMEM((3, 8, 128), F32),
            pltpu.VMEM((3, 8, 128), F32),
            pltpu.VMEM((NH, ROWS // 2, 128), BF),
            pltpu.VMEM((NH - 1, ROWS // 2, 128), BF),
            pltpu.VMEM((NH * HD, D), BF),
            dma((3,)), dma((3,)),
            dma((28,)), dma((28,)),
            dma((19,)), dma((32,)),
            dma((3,)), dma((3,)),
            dma((3,)), dma((3,)),
            dma((15,)), dma((15,)),
            dma((9,)),
            pltpu.SemaphoreType.REGULAR((2,)),
        ],
        compiler_params=pltpu.CompilerParams(
            collective_id=0, has_side_effects=True, vmem_limit_bytes=60 * 1024 * 1024
        ),
        name="joint_attention",
    )(
        queries.T, key_rows.T, values.T, text_keys.T, text_values.T,
        block_image, gate_image, residual, w_out,
    )


def solution(mesh):
    placed = (
        P("blk", "head"),
        P("blk", "head"),
        P("blk", "head"),
        P(None, "head"),
        P(None, "head"),
        P(),
        P(),
        P(("blk", "head"), None),
        P("head", None),
    )
    return jax.shard_map(
        on_device, mesh=mesh, in_specs=placed, out_specs=P(("blk", "head"), None), check_vma=False
    )
```

```python
import functools
import math

import jax
import jax.numpy as jnp
from jax import lax
from jax.experimental import pallas as pl
from jax.experimental.pallas import tpu as pltpu
from jax.sharding import PartitionSpec as P

HD = 64
TEXT = 154
BS = 128
TOK = 512
YL = 4
ZL = 8
NH = 16
D = 1536
ROWS = TOK // NH
TSLOTS = 3
FAR = -(2.0**100)
RATE = math.log2(math.e) / math.sqrt(HD)
MESH = pl.DeviceIdType.MESH
BF = jnp.bfloat16
F32 = jnp.float32
NT = (((1,), (1,)), ((), ()))


def flip(index, mask, bits):
    total = 0
    for b in range(bits):
        bit = lax.rem(lax.div(index, 1 << b), 2)
        total = total + (1 << b) * ((1 - bit) if (mask >> b) & 1 else bit)
    return total


def iota(shape, dim):
    return lax.broadcasted_iota(jnp.int32, shape, dim)


def kernel(
    q_hbm, k_hbm, v_hbm, tk_hbm, tv_hbm, img_hbm, gate_hbm, res_hbm, w_hbm,
    out_ref,
    img_ref, kv, qt, tk_ref, tv_ref, gate_ref, res_ref, qa, ka, va, acc, mx, tpad, s0, s1, osend, orecv, ssend, srecv, packed, arecv, wbuf,
    q_s, q_r, kv_s, kv_r, w_s, w_r, o_s, o_r, st_s, st_r, a_s, a_r, in_s, token,
):
    blk = lax.axis_index("blk")
    head = lax.axis_index("head")
    z = lax.div(blk, YL)
    y = lax.rem(blk, YL)
    zright = lax.rem(z + 1, ZL) * YL + y
    zleft = lax.rem(z + ZL - 1, ZL) * YL + y
    ypeer = [z * YL + flip(y, c, 2) for c in range(YL)]
    hpeer = [flip(head, s, 4) for s in range(NH)]

    barrier = pltpu.get_barrier_semaphore()
    for other in (zright, zleft, ypeer[1], ypeer[2], ypeer[3]):
        pl.semaphore_signal(barrier, inc=1, device_id={"blk": other}, device_id_type=MESH)
    for s in (4, 12, 8, 2, 1):
        pl.semaphore_signal(barrier, inc=1, device_id={"head": hpeer[s]}, device_id_type=MESH)

    loads = [
        pltpu.make_async_copy(src, dst, in_s.at[n])
        for n, (src, dst) in enumerate((
            (img_hbm, img_ref),
            (q_hbm, qt.at[0]),
            (k_hbm, kv.at[0, pl.ds(0, HD)]),
            (v_hbm, kv.at[0, pl.ds(HD, HD)]),
            (w_hbm, wbuf.at[pl.ds(0, HD)]),
            (tk_hbm, tk_ref),
            (tv_hbm, tv_ref),
            (gate_hbm, gate_ref),
            (res_hbm, res_ref),
        ))
    ]
    for cp in loads:
        cp.start()

    def send(src, dst, ssem, rsem, dev):
        copy = pltpu.make_async_remote_copy(
            src_ref=src, dst_ref=dst, send_sem=ssem, recv_sem=rsem,
            device_id=dev, device_id_type=MESH,
        )
        copy.start()
        return copy

    def settle(ref, sem, sent=False):
        copy = pltpu.make_async_remote_copy(
            src_ref=ref, dst_ref=ref, send_sem=sem, recv_sem=sem,
            device_id={"head": hpeer[1]}, device_id_type=MESH,
        )
        if sent:
            copy.wait_send()
        else:
            copy.wait_recv()

    def q_copy(c):
        return send(qt.at[0], qt.at[c], q_s, q_r.at[c - 1], {"blk": ypeer[c]})

    kv_cps = {}

    def kv_send(kind, step, half):
        src = step - 1 if kind in ("lk", "lv") or step == 1 else ZL - (step - 1)
        dst = step if kind in ("lk", "lv") else ZL - step
        k = 2 * ({"rk": 0, "rv": 4, "lk": 7, "lv": 10}[kind] + step - 1) + half
        rows = pl.ds((0 if kind in ("rk", "lk") else HD) + half * (HD // 2), HD // 2)
        dev = {"blk": zleft if kind in ("lk", "lv") else zright}
        kv_cps[kind, step, half] = send(kv.at[src, rows], kv.at[dst, rows], kv_s, kv_r.at[k], dev)

    def kv_hop(part, step):
        for half in range(2):
            for kind in ("r" + part, "l" + part):
                if (kind, step, half) in kv_cps:
                    kv_cps[kind, step, half].wait_recv()
                    if step < {"rk": 4, "lk": 3, "rv": 3, "lv": 4}[kind]:
                        kv_send(kind, step + 1, half)

    def w_part(slot, half):
        if half is None:
            return wbuf.at[pl.ds(slot * HD, HD)]
        return wbuf.at[pl.ds(slot * HD + half * (HD // 2), HD // 2)]

    def w_copy(origin, to, half=None):
        slot = origin ^ to
        if slot == 2:
            sem = w_r.at[half]
        elif slot % 2:
            sem = w_r.at[2]
        else:
            sem = w_r.at[3 if slot in (4, 12, 8) else 4]
        send(w_part(origin, half), w_part(slot, half), w_s, sem, {"head": hpeer[to]})

    def fill_keys(slot, first_block):
        row = iota((HD, BS), 0)
        gaps = []
        for b in range(TOK // BS):
            image = img_ref[first_block + b]
            gaps.append(jnp.where((row < 8) & (row != image), FAR, 0.0))
        wide = jnp.concatenate([kv[slot, 0:HD].astype(F32), jnp.concatenate(gaps, axis=1)], axis=0)
        ka[slot] = wide.T.astype(BF)
        va[slot, 0:HD] = kv[slot, HD : 2 * HD]
        va[slot, HD : HD + 16] = jnp.ones((16, TOK), BF)

    def fill_queries(c):
        qa[c, 0:HD] = qt[c]
        first = ypeer[c] * (TOK // BS)
        for b in range(TOK // BS):
            image = img_ref[first + b]
            hot = (iota((16, BS), 0) == image).astype(F32)
            qa[c, HD : HD + 16, b * BS : (b + 1) * BS] = hot.astype(BF)
        qa[c, HD + 16 : 128] = jnp.zeros((128 - HD - 16, TOK), BF)

    seen = set()
    pending = []
    turn = [0]

    def scores(slot, c, n, buf):
        sc = jnp.dot(ka[slot, 0:n], qa[c], preferred_element_type=F32)
        buf[0:n] = sc
        buf[TOK : TOK + 8] = jnp.max(sc.reshape(n // 8, 8, TOK), axis=0)

    def soften(slot, c, n, buf):
        new = jnp.max(buf[TOK : TOK + 8], axis=0, keepdims=True)
        if c in seen:
            old = mx[c, 0:1]
            new = jnp.maximum(old, new)
            shrink = jnp.exp2((old - new) * RATE)
        pr = jnp.exp2((buf[0:n] - new) * RATE).astype(BF)
        upd = jnp.dot(va[slot, :, 0:n], pr, preferred_element_type=F32)
        if c in seen:
            acc[c] = acc[c] * shrink + upd
        else:
            acc[c] = upd
        mx[c, 0:1] = new
        seen.add(c)

    def flush():
        while pending:
            soften(*pending.pop(0))

    def steps(*pairs):
        for slot, c in pairs:
            n = tail if slot == ZL + TSLOTS - 1 else TOK
            buf = (s0, s1)[turn[0] % 2]
            turn[0] += 1
            scores(slot, c, n, buf)
            flush()
            pending.append((slot, c, n, buf))

    def origin_block(slot):
        return (lax.rem(z + slot, ZL) * YL + y) * (TOK // BS)

    def send_part(c):
        osend[c - 1] = acc[c, 0:HD].astype(BF)
        for a in range(4):
            ssend[c - 1, a : a + 1] = mx[c, 0:1, a * 128 : (a + 1) * 128]
            ssend[c - 1, 4 + a : 5 + a] = acc[c, HD : HD + 1, a * 128 : (a + 1) * 128]
        dev = {"blk": ypeer[c]}
        send(osend.at[c - 1], orecv.at[c - 1], o_s, o_r, dev)
        send(ssend.at[c - 1], srecv.at[c - 1], st_s, st_r, dev)

    ntext = tk_hbm.shape[1]
    edge = (TSLOTS - 1) * TOK
    tail = -(-(ntext - edge) // 128) * 128
    for cp in loads[:4]:
        cp.wait()
    with jax.named_scope("barrier"):
        pl.semaphore_wait(barrier, 10)

    q_cps = [None] + [q_copy(c) for c in (1, 2, 3)]
    for part in ("k", "v"):
        for half in range(2):
            kv_send("r" + part, 1, half)
            kv_send("l" + part, 1, half)
    pl.semaphore_signal(token.at[0], inc=1, device_id={"head": hpeer[2]}, device_id_type=MESH)
    loads[4].wait()
    for s in (4, 12, 8):
        w_copy(0, s)
    w_copy(0, 1)

    fill_queries(0)
    fill_keys(0, blk * (TOK // BS))
    loads[5].wait()
    loads[6].wait()
    for n, ref in ((0, tk_ref), (1, tv_ref)):
        tpad[n, :, edge:] = jnp.zeros((HD, TOK), BF)
        tpad[n, :, 0:ntext] = ref[...]
    for t in range(TSLOTS):
        row = iota((HD, TOK), 0)
        col = iota((HD, TOK), 1) + t * TOK
        inside = (col >= row * TEXT) & (col < (row + 1) * TEXT)
        gap = jnp.where((row < 8) & jnp.logical_not(inside), FAR, 0.0)
        span = slice(t * TOK, (t + 1) * TOK)
        wide = jnp.concatenate([tpad[0, :, span].astype(F32), gap], axis=0)
        ka[ZL + t] = wide.T.astype(BF)
        va[ZL + t, 0:HD] = tpad[1, :, span]
        va[ZL + t, HD : HD + 16] = jnp.ones((16, TOK), BF)

    with jax.named_scope("text"):
        steps((8, 0), (9, 0), (10, 0), (0, 0))
        flush()
    with jax.named_scope("k1"):
        kv_hop("k", 1)
    with jax.named_scope("v1"):
        kv_hop("v", 1)
    fill_keys(7, origin_block(7))
    fill_keys(1, origin_block(1))
    steps((7, 0), (1, 0))
    with jax.named_scope("qwait1"):
        q_cps[1].wait_recv()
    w_copy(0, 2, 0)
    pl.semaphore_wait(token.at[0], 1)
    pl.semaphore_signal(token.at[1], inc=1, device_id={"head": hpeer[1]}, device_id_type=MESH)
    fill_queries(1)
    steps((0, 1), (7, 1), (1, 1))
    with jax.named_scope("k2"):
        kv_hop("k", 2)
    with jax.named_scope("qwait2"):
        q_cps[2].wait_recv()
    w_copy(0, 2, 1)
    fill_queries(2)
    steps((0, 2), (7, 2), (1, 2))
    with jax.named_scope("v2"):
        kv_hop("v", 2)
    fill_keys(6, origin_block(6))
    fill_keys(2, origin_block(2))
    steps((6, 1), (2, 1), (6, 2), (2, 2))
    with jax.named_scope("k3"):
        kv_hop("k", 3)
    steps((6, 0), (2, 0))
    with jax.named_scope("v3"):
        kv_hop("v", 3)
    fill_keys(5, origin_block(5))
    fill_keys(3, origin_block(3))
    steps((5, 1), (3, 1))
    with jax.named_scope("qwait3"):
        q_cps[3].wait_recv()
    fill_queries(3)
    steps((0, 3), (7, 3))
    with jax.named_scope("k4"):
        kv_hop("k", 4)
    settle(wbuf.at[pl.ds(0, 3 * HD)], w_r.at[3])
    for s in (4, 12, 8):
        w_copy(s, 1)
    steps((1, 3), (6, 3), (2, 3))
    with jax.named_scope("v4"):
        kv_hop("v", 4)
    fill_keys(4, origin_block(4))
    steps((5, 3), (3, 3))
    with jax.named_scope("wywait"):
        settle(w_part(2, 0), w_r.at[0])
    for s in (4, 12, 8):
        w_copy(2, s, 0)
    steps((4, 3), (5, 2))
    send_part(3)
    steps((3, 2), (4, 2), (4, 1))
    send_part(2)
    with jax.named_scope("wywait2"):
        settle(w_part(2, 1), w_r.at[1])
    for s in (4, 12, 8):
        w_copy(2, s, 1)
    w_copy(2, 1)
    steps((5, 0))
    send_part(1)
    steps((3, 0), (4, 0))
    flush()
    pl.semaphore_wait(token.at[1], 1)
    with jax.named_scope("owait"):
        settle(orecv, o_r)
        settle(srecv, st_r)

    def row_of(ref, c, first):
        return jnp.concatenate([ref[c - 1, first + a : first + a + 1] for a in range(4)], axis=1)

    maxes = [mx[0, 0:1]] + [row_of(srecv, c, 0) for c in (1, 2, 3)]
    sums = [acc[0, HD : HD + 1]] + [row_of(srecv, c, 4) for c in (1, 2, 3)]
    top = functools.reduce(jnp.maximum, maxes)
    scales = [jnp.exp2((m - top) * RATE) for m in maxes]
    denom = functools.reduce(jnp.add, [s * l for s, l in zip(scales, sums)])
    numer = acc[0, 0:HD] * scales[0]
    for c in (1, 2, 3):
        numer = numer + orecv[c - 1].astype(F32) * scales[c]
    att = numer / denom
    both = jnp.concatenate([att, att], axis=0).T
    half = ROWS // 2
    side = iota((half, 128), 1) < HD
    for j in range(NH):
        one = both[j * ROWS : j * ROWS + half]
        two = both[j * ROWS + half : (j + 1) * ROWS]
        packed[j] = jnp.where(side, one, two).astype(BF)

    for s in (10, 11, 2, 3, 6, 7, 14, 15, 8, 9, 4, 5, 12, 13, 1):
        send(packed.at[hpeer[s]], arecv.at[s - 1], a_s, a_r, {"head": hpeer[s]})
    with jax.named_scope("wxwait2"):
        settle(wbuf.at[pl.ds(0, 3 * HD)], w_r.at[4])
    for s in (6, 14, 10):
        w_copy(s, 1)
    mine = packed[head].astype(F32)
    with jax.named_scope("await"):
        settle(arecv, a_r)
    loads[7].wait()
    loads[8].wait()
    with jax.named_scope("wcwait"):
        settle(wbuf.at[pl.ds(0, NH // 2 * HD)], w_r.at[2])
    pairs = []
    for i in range(NH // 2):
        even = mine if i == 0 else arecv[2 * i - 1].astype(F32)
        odd = arecv[2 * i].astype(F32)
        upper = jnp.where(side, even, pltpu.roll(odd, HD, 1))
        lower = jnp.where(side, pltpu.roll(even, HD, 1), odd)
        pairs.append(jnp.concatenate([upper, lower], axis=0).astype(BF))
    mixed = jnp.concatenate(pairs, axis=1)
    image = img_ref[blk * (TOK // BS) + lax.div(head, NH * BS // TOK)]
    gating = gate_ref[pl.ds(image, 1), :]
    projected = jnp.dot(mixed, wbuf[...], preferred_element_type=F32)
    out_ref[...] = (res_ref[...].astype(F32) + gating * projected).astype(BF)
    with jax.named_scope("sendwait"):
        settle(qt.at[pl.ds(1, 3)], q_s, True)
        settle(kv.at[pl.ds(0, 7)], kv_s, True)
        settle(wbuf.at[pl.ds(0, 15 * HD)], w_s, True)
        settle(osend, o_s, True)
        settle(ssend, st_s, True)
        settle(arecv, a_s, True)


def on_device(queries, key_rows, values, text_keys, text_values, block_image, gate_image, residual, w_out):
    vm = pl.BlockSpec(memory_space=pltpu.VMEM)
    hb = pl.BlockSpec(memory_space=pl.ANY)
    dma = pltpu.SemaphoreType.DMA
    return pl.pallas_call(
        kernel,
        out_shape=pltpu.VMEM((ROWS, D), BF),
        in_specs=[hb] * 9,
        out_specs=vm,
        scratch_shapes=[
            pltpu.SMEM(block_image.shape, jnp.int32),
            pltpu.VMEM((ZL, 2 * HD, TOK), BF),
            pltpu.VMEM((YL, HD, TOK), BF),
            pltpu.VMEM((HD, text_keys.shape[0]), BF),
            pltpu.VMEM((HD, text_keys.shape[0]), BF),
            pltpu.VMEM(gate_image.shape, F32),
            pltpu.VMEM((ROWS, D), BF),
            pltpu.VMEM((YL, 128, TOK), BF),
            pltpu.VMEM((ZL + TSLOTS, TOK, 128), BF),
            pltpu.VMEM((ZL + TSLOTS, HD + 16, TOK), BF),
            pltpu.VMEM((YL, HD + 16, TOK), F32),
            pltpu.VMEM((YL, 8, TOK), F32),
            pltpu.VMEM((2, HD, TSLOTS * TOK), BF),
            pltpu.VMEM((TOK + 8, TOK), F32),
            pltpu.VMEM((TOK + 8, TOK), F32),
            pltpu.VMEM((3, HD, TOK), BF),
            pltpu.VMEM((3, HD, TOK), BF),
            pltpu.VMEM((3, 8, 128), F32),
            pltpu.VMEM((3, 8, 128), F32),
            pltpu.VMEM((NH, ROWS // 2, 128), BF),
            pltpu.VMEM((NH - 1, ROWS // 2, 128), BF),
            pltpu.VMEM((NH * HD, D), BF),
            dma, dma((3,)),
            dma, dma((28,)),
            dma, dma((5,)),
            dma, dma,
            dma, dma,
            dma, dma,
            dma((9,)),
            pltpu.SemaphoreType.REGULAR((2,)),
        ],
        compiler_params=pltpu.CompilerParams(
            collective_id=0, has_side_effects=True, vmem_limit_bytes=60 * 1024 * 1024
        ),
        name="joint_attention",
    )(
        queries.T, key_rows.T, values.T, text_keys.T, text_values.T,
        block_image, gate_image, residual, w_out,
    )


def solution(mesh):
    placed = (
        P("blk", "head"),
        P("blk", "head"),
        P("blk", "head"),
        P(None, "head"),
        P(None, "head"),
        P(),
        P(),
        P(("blk", "head"), None),
        P("head", None),
    )
    return jax.shard_map(
        on_device, mesh=mesh, in_specs=placed, out_specs=P(("blk", "head"), None), check_vma=False
    )
```

```python
import functools
import math

import jax
import jax.numpy as jnp
from jax import lax
from jax.experimental import pallas as pl
from jax.experimental.pallas import tpu as pltpu
from jax.sharding import PartitionSpec as P

HD = 64
TEXT = 154
BS = 128
TOK = 512
YL = 4
ZL = 8
NH = 16
D = 1536
ROWS = TOK // NH
TSLOTS = 3
WQ = 4
FAR = -(2.0**100)
RATE = math.log2(math.e) / math.sqrt(HD)
MESH = pl.DeviceIdType.MESH
BF = jnp.bfloat16
F32 = jnp.float32
NT = (((1,), (1,)), ((), ()))


def flip(index, mask, bits):
    total = 0
    for b in range(bits):
        bit = lax.rem(lax.div(index, 1 << b), 2)
        total = total + (1 << b) * ((1 - bit) if (mask >> b) & 1 else bit)
    return total


def iota(shape, dim):
    return lax.broadcasted_iota(jnp.int32, shape, dim)


def kernel(
    q_hbm, k_hbm, v_hbm, tk_hbm, tv_hbm, img_hbm, gate_hbm, res_hbm, w_hbm,
    out_ref,
    img_ref, kv, qt, tk_ref, tv_ref, gate_ref, res_ref, qa, ka, va, acc, mx, tpad, s0, s1, osend, orecv, ssend, srecv, packed, arecv, wbuf,
    q_s, q_r, kv_s, kv_r, w_s, w_r, o_s, o_r, st_s, st_r, a_s, a_r, in_s, token,
):
    blk = lax.axis_index("blk")
    head = lax.axis_index("head")
    z = lax.div(blk, YL)
    y = lax.rem(blk, YL)
    zright = lax.rem(z + 1, ZL) * YL + y
    zleft = lax.rem(z + ZL - 1, ZL) * YL + y
    ypeer = [z * YL + flip(y, c, 2) for c in range(YL)]
    hpeer = [flip(head, s, 4) for s in range(NH)]

    barrier = pltpu.get_barrier_semaphore()
    for other in (zright, zleft, ypeer[1], ypeer[2], ypeer[3]):
        pl.semaphore_signal(barrier, inc=1, device_id={"blk": other}, device_id_type=MESH)
    for s in (4, 12, 8, 2, 1):
        pl.semaphore_signal(barrier, inc=1, device_id={"head": hpeer[s]}, device_id_type=MESH)

    loads = [
        pltpu.make_async_copy(src, dst, in_s.at[n])
        for n, (src, dst) in enumerate((
            (img_hbm, img_ref),
            (q_hbm, qt.at[0]),
            (k_hbm, kv.at[0, pl.ds(0, HD)]),
            (v_hbm, kv.at[0, pl.ds(HD, HD)]),
            (w_hbm, wbuf.at[pl.ds(0, HD)]),
            (tk_hbm, tk_ref),
            (tv_hbm, tv_ref),
            (gate_hbm, gate_ref),
            (res_hbm, res_ref),
        ))
    ]
    for cp in loads:
        cp.start()

    def send(src, dst, ssem, rsem, dev):
        copy = pltpu.make_async_remote_copy(
            src_ref=src, dst_ref=dst, send_sem=ssem, recv_sem=rsem,
            device_id=dev, device_id_type=MESH,
        )
        copy.start()
        return copy

    def settle(ref, sem, sent=False):
        copy = pltpu.make_async_remote_copy(
            src_ref=ref, dst_ref=ref, send_sem=sem, recv_sem=sem,
            device_id={"head": hpeer[1]}, device_id_type=MESH,
        )
        if sent:
            copy.wait_send()
        else:
            copy.wait_recv()

    def q_copy(c):
        return send(qt.at[0], qt.at[c], q_s, q_r.at[c - 1], {"blk": ypeer[c]})

    kv_cps = {}

    def kv_send(kind, step, half):
        src = step - 1 if kind in ("lk", "lv") or step == 1 else ZL - (step - 1)
        dst = step if kind in ("lk", "lv") else ZL - step
        k = 2 * ({"rk": 0, "rv": 4, "lk": 7, "lv": 10}[kind] + step - 1) + half
        rows = pl.ds((0 if kind in ("rk", "lk") else HD) + half * (HD // 2), HD // 2)
        dev = {"blk": zleft if kind in ("lk", "lv") else zright}
        kv_cps[kind, step, half] = send(kv.at[src, rows], kv.at[dst, rows], kv_s, kv_r.at[k], dev)

    def kv_hop(part, step):
        for half in range(2):
            for kind in ("r" + part, "l" + part):
                if (kind, step, half) in kv_cps:
                    kv_cps[kind, step, half].wait_recv()
                    if step < {"rk": 4, "lk": 3, "rv": 3, "lv": 4}[kind]:
                        kv_send(kind, step + 1, half)

    def w_part(slot, half):
        if half is None:
            return wbuf.at[pl.ds(slot * HD, HD)]
        return wbuf.at[pl.ds(slot * HD + half * (HD // WQ), HD // WQ)]

    def w_copy(origin, to, half=None):
        slot = origin ^ to
        if slot == 2:
            sem = w_r.at[half]
        elif slot % 2:
            sem = w_r.at[WQ]
        else:
            sem = w_r.at[WQ + 1 if slot in (4, 12, 8) else WQ + 2]
        send(w_part(origin, half), w_part(slot, half), w_s, sem, {"head": hpeer[to]})

    def fill_keys(slot, first_block):
        row = iota((HD, BS), 0)
        gaps = []
        for b in range(TOK // BS):
            image = img_ref[first_block + b]
            gaps.append(jnp.where((row < 8) & (row != image), FAR, 0.0))
        wide = jnp.concatenate([kv[slot, 0:HD].astype(F32), jnp.concatenate(gaps, axis=1)], axis=0)
        ka[slot] = wide.T.astype(BF)
        va[slot, 0:HD] = kv[slot, HD : 2 * HD]
        va[slot, HD : HD + 16] = jnp.ones((16, TOK), BF)

    def fill_queries(c):
        qa[c, 0:HD] = qt[c]
        first = ypeer[c] * (TOK // BS)
        for b in range(TOK // BS):
            image = img_ref[first + b]
            hot = (iota((16, BS), 0) == image).astype(F32)
            qa[c, HD : HD + 16, b * BS : (b + 1) * BS] = hot.astype(BF)
        qa[c, HD + 16 : 128] = jnp.zeros((128 - HD - 16, TOK), BF)

    seen = set()
    pending = []
    turn = [0]

    def scores(slot, c, n, buf):
        sc = jnp.dot(ka[slot, 0:n], qa[c], preferred_element_type=F32)
        buf[0:n] = sc
        buf[TOK : TOK + 8] = jnp.max(sc.reshape(n // 8, 8, TOK), axis=0)

    def soften(slot, c, n, buf):
        new = jnp.max(buf[TOK : TOK + 8], axis=0, keepdims=True)
        if c in seen:
            old = mx[c, 0:1]
            new = jnp.maximum(old, new)
            shrink = jnp.exp2((old - new) * RATE)
        pr = jnp.exp2((buf[0:n] - new) * RATE).astype(BF)
        upd = jnp.dot(va[slot, :, 0:n], pr, preferred_element_type=F32)
        if c in seen:
            acc[c] = acc[c] * shrink + upd
        else:
            acc[c] = upd
        mx[c, 0:1] = new
        seen.add(c)

    def flush():
        while pending:
            soften(*pending.pop(0))

    def steps(*pairs):
        for slot, c in pairs:
            n = tail if slot == ZL + TSLOTS - 1 else TOK
            buf = (s0, s1)[turn[0] % 2]
            turn[0] += 1
            scores(slot, c, n, buf)
            flush()
            pending.append((slot, c, n, buf))

    def origin_block(slot):
        return (lax.rem(z + slot, ZL) * YL + y) * (TOK // BS)

    def send_part(c):
        osend[c - 1] = acc[c, 0:HD].astype(BF)
        for a in range(4):
            ssend[c - 1, a : a + 1] = mx[c, 0:1, a * 128 : (a + 1) * 128]
            ssend[c - 1, 4 + a : 5 + a] = acc[c, HD : HD + 1, a * 128 : (a + 1) * 128]
        dev = {"blk": ypeer[c]}
        send(osend.at[c - 1], orecv.at[c - 1], o_s, o_r, dev)
        send(ssend.at[c - 1], srecv.at[c - 1], st_s, st_r, dev)

    ntext = tk_hbm.shape[1]
    edge = (TSLOTS - 1) * TOK
    tail = -(-(ntext - edge) // 128) * 128
    for cp in loads[:4]:
        cp.wait()
    with jax.named_scope("barrier"):
        pl.semaphore_wait(barrier, 10)

    q_cps = [None] + [q_copy(c) for c in (1, 2, 3)]
    for part in ("k", "v"):
        for half in range(2):
            kv_send("r" + part, 1, half)
            kv_send("l" + part, 1, half)
    pl.semaphore_signal(token.at[0], inc=1, device_id={"head": hpeer[2]}, device_id_type=MESH)
    loads[4].wait()
    for s in (4, 12, 8):
        w_copy(0, s)
    w_copy(0, 1)

    fill_queries(0)
    fill_keys(0, blk * (TOK // BS))
    loads[5].wait()
    loads[6].wait()
    for n, ref in ((0, tk_ref), (1, tv_ref)):
        tpad[n, :, edge:] = jnp.zeros((HD, TOK), BF)
        tpad[n, :, 0:ntext] = ref[...]
    for t in range(TSLOTS):
        row = iota((HD, TOK), 0)
        col = iota((HD, TOK), 1) + t * TOK
        inside = (col >= row * TEXT) & (col < (row + 1) * TEXT)
        gap = jnp.where((row < 8) & jnp.logical_not(inside), FAR, 0.0)
        span = slice(t * TOK, (t + 1) * TOK)
        wide = jnp.concatenate([tpad[0, :, span].astype(F32), gap], axis=0)
        ka[ZL + t] = wide.T.astype(BF)
        va[ZL + t, 0:HD] = tpad[1, :, span]
        va[ZL + t, HD : HD + 16] = jnp.ones((16, TOK), BF)

    with jax.named_scope("text"):
        steps((8, 0), (9, 0), (10, 0), (0, 0))
        flush()
    with jax.named_scope("k1"):
        kv_hop("k", 1)
    with jax.named_scope("v1"):
        kv_hop("v", 1)
    fill_keys(7, origin_block(7))
    fill_keys(1, origin_block(1))
    steps((7, 0), (1, 0))
    with jax.named_scope("qwait1"):
        q_cps[1].wait_recv()
    w_copy(0, 2, 0)
    pl.semaphore_wait(token.at[0], 1)
    pl.semaphore_signal(token.at[1], inc=1, device_id={"head": hpeer[1]}, device_id_type=MESH)
    fill_queries(1)
    steps((0, 1), (7, 1), (1, 1))
    with jax.named_scope("k2"):
        kv_hop("k", 2)
    with jax.named_scope("qwait2"):
        q_cps[2].wait_recv()
    w_copy(0, 2, 1)
    fill_queries(2)
    steps((0, 2), (7, 2), (1, 2))
    with jax.named_scope("v2"):
        kv_hop("v", 2)
    w_copy(0, 2, 2)
    fill_keys(6, origin_block(6))
    fill_keys(2, origin_block(2))
    steps((6, 1), (2, 1), (6, 2), (2, 2))
    with jax.named_scope("k3"):
        kv_hop("k", 3)
    w_copy(0, 2, 3)
    with jax.named_scope("qwait3"):
        q_cps[3].wait_recv()
    fill_queries(3)
    steps((0, 3), (7, 3))
    steps((1, 3))
    with jax.named_scope("v3"):
        kv_hop("v", 3)
    fill_keys(5, origin_block(5))
    fill_keys(3, origin_block(3))
    steps((5, 1), (3, 1), (6, 3), (2, 3))
    def w_hop(quarter):
        with jax.named_scope("wy%d" % quarter):
            settle(w_part(2, quarter), w_r.at[quarter])
        for s in (4, 12, 8):
            w_copy(2, s, quarter)

    with jax.named_scope("k4"):
        kv_hop("k", 4)
    settle(wbuf.at[pl.ds(0, 3 * HD)], w_r.at[WQ + 1])
    for s in (4, 12, 8):
        w_copy(s, 1)
    w_hop(0)
    steps((5, 3), (3, 3))
    with jax.named_scope("v4"):
        kv_hop("v", 4)
    w_hop(1)
    fill_keys(4, origin_block(4))
    steps((4, 3), (5, 2))
    send_part(3)
    w_hop(2)
    steps((3, 2), (4, 2), (4, 1))
    send_part(2)
    w_hop(3)
    w_copy(2, 1)
    steps((5, 0))
    send_part(1)
    steps((3, 0), (4, 0), (6, 0), (2, 0))
    flush()
    pl.semaphore_wait(token.at[1], 1)
    with jax.named_scope("owait"):
        settle(orecv, o_r)
        settle(srecv, st_r)

    def row_of(ref, c, first):
        return jnp.concatenate([ref[c - 1, first + a : first + a + 1] for a in range(4)], axis=1)

    maxes = [mx[0, 0:1]] + [row_of(srecv, c, 0) for c in (1, 2, 3)]
    sums = [acc[0, HD : HD + 1]] + [row_of(srecv, c, 4) for c in (1, 2, 3)]
    top = functools.reduce(jnp.maximum, maxes)
    scales = [jnp.exp2((m - top) * RATE) for m in maxes]
    denom = functools.reduce(jnp.add, [s * l for s, l in zip(scales, sums)])
    numer = acc[0, 0:HD] * scales[0]
    for c in (1, 2, 3):
        numer = numer + orecv[c - 1].astype(F32) * scales[c]
    att = numer / denom
    both = jnp.concatenate([att, att], axis=0).T
    half = ROWS // 2
    side = iota((half, 128), 1) < HD
    for j in range(NH):
        one = both[j * ROWS : j * ROWS + half]
        two = both[j * ROWS + half : (j + 1) * ROWS]
        packed[j] = jnp.where(side, one, two).astype(BF)

    for s in (10, 11, 2, 3, 6, 7, 14, 15, 8, 9, 4, 5, 12, 13, 1):
        send(packed.at[hpeer[s]], arecv.at[s - 1], a_s, a_r, {"head": hpeer[s]})
    with jax.named_scope("wxwait2"):
        settle(wbuf.at[pl.ds(0, 3 * HD)], w_r.at[WQ + 2])
    for s in (6, 14, 10):
        w_copy(s, 1)
    mine = packed[head].astype(F32)
    with jax.named_scope("await"):
        settle(arecv, a_r)
    loads[7].wait()
    loads[8].wait()
    with jax.named_scope("wcwait"):
        settle(wbuf.at[pl.ds(0, NH // 2 * HD)], w_r.at[WQ])
    pairs = []
    for i in range(NH // 2):
        even = mine if i == 0 else arecv[2 * i - 1].astype(F32)
        odd = arecv[2 * i].astype(F32)
        upper = jnp.where(side, even, pltpu.roll(odd, HD, 1))
        lower = jnp.where(side, pltpu.roll(even, HD, 1), odd)
        pairs.append(jnp.concatenate([upper, lower], axis=0).astype(BF))
    mixed = jnp.concatenate(pairs, axis=1)
    image = img_ref[blk * (TOK // BS) + lax.div(head, NH * BS // TOK)]
    gating = gate_ref[pl.ds(image, 1), :]
    projected = jnp.dot(mixed, wbuf[...], preferred_element_type=F32)
    out_ref[...] = (res_ref[...].astype(F32) + gating * projected).astype(BF)
    with jax.named_scope("sendwait"):
        settle(qt.at[pl.ds(1, 3)], q_s, True)
        settle(kv.at[pl.ds(0, 7)], kv_s, True)
        settle(wbuf.at[pl.ds(0, 15 * HD)], w_s, True)
        settle(osend, o_s, True)
        settle(ssend, st_s, True)
        settle(arecv, a_s, True)


def on_device(queries, key_rows, values, text_keys, text_values, block_image, gate_image, residual, w_out):
    vm = pl.BlockSpec(memory_space=pltpu.VMEM)
    hb = pl.BlockSpec(memory_space=pl.ANY)
    dma = pltpu.SemaphoreType.DMA
    return pl.pallas_call(
        kernel,
        out_shape=pltpu.VMEM((ROWS, D), BF),
        in_specs=[hb] * 9,
        out_specs=vm,
        scratch_shapes=[
            pltpu.SMEM(block_image.shape, jnp.int32),
            pltpu.VMEM((ZL, 2 * HD, TOK), BF),
            pltpu.VMEM((YL, HD, TOK), BF),
            pltpu.VMEM((HD, text_keys.shape[0]), BF),
            pltpu.VMEM((HD, text_keys.shape[0]), BF),
            pltpu.VMEM(gate_image.shape, F32),
            pltpu.VMEM((ROWS, D), BF),
            pltpu.VMEM((YL, 128, TOK), BF),
            pltpu.VMEM((ZL + TSLOTS, TOK, 128), BF),
            pltpu.VMEM((ZL + TSLOTS, HD + 16, TOK), BF),
            pltpu.VMEM((YL, HD + 16, TOK), F32),
            pltpu.VMEM((YL, 8, TOK), F32),
            pltpu.VMEM((2, HD, TSLOTS * TOK), BF),
            pltpu.VMEM((TOK + 8, TOK), F32),
            pltpu.VMEM((TOK + 8, TOK), F32),
            pltpu.VMEM((3, HD, TOK), BF),
            pltpu.VMEM((3, HD, TOK), BF),
            pltpu.VMEM((3, 8, 128), F32),
            pltpu.VMEM((3, 8, 128), F32),
            pltpu.VMEM((NH, ROWS // 2, 128), BF),
            pltpu.VMEM((NH - 1, ROWS // 2, 128), BF),
            pltpu.VMEM((NH * HD, D), BF),
            dma, dma((3,)),
            dma, dma((28,)),
            dma, dma((WQ + 3,)),
            dma, dma,
            dma, dma,
            dma, dma,
            dma((9,)),
            pltpu.SemaphoreType.REGULAR((2,)),
        ],
        compiler_params=pltpu.CompilerParams(
            collective_id=0, has_side_effects=True, vmem_limit_bytes=60 * 1024 * 1024
        ),
        name="joint_attention",
    )(
        queries.T, key_rows.T, values.T, text_keys.T, text_values.T,
        block_image, gate_image, residual, w_out,
    )


def solution(mesh):
    placed = (
        P("blk", "head"),
        P("blk", "head"),
        P("blk", "head"),
        P(None, "head"),
        P(None, "head"),
        P(),
        P(),
        P(("blk", "head"), None),
        P("head", None),
    )
    return jax.shard_map(
        on_device, mesh=mesh, in_specs=placed, out_specs=P(("blk", "head"), None), check_vma=False
    )
```

```python
import functools
import math

import jax
import jax.numpy as jnp
from jax import lax
from jax.experimental import pallas as pl
from jax.experimental.pallas import tpu as pltpu
from jax.sharding import PartitionSpec as P

HD = 64
TEXT = 154
BS = 128
TOK = 512
YL = 4
ZL = 8
NH = 16
D = 1536
ROWS = TOK // NH
TSLOTS = 3
WQ = 4
FAR = -(2.0**100)
RATE = math.log2(math.e) / math.sqrt(HD)
MESH = pl.DeviceIdType.MESH
BF = jnp.bfloat16
F32 = jnp.float32
NT = (((1,), (1,)), ((), ()))


def flip(index, mask, bits):
    total = 0
    for b in range(bits):
        bit = lax.rem(lax.div(index, 1 << b), 2)
        total = total + (1 << b) * ((1 - bit) if (mask >> b) & 1 else bit)
    return total


def iota(shape, dim):
    return lax.broadcasted_iota(jnp.int32, shape, dim)


def kernel(
    q_hbm, k_hbm, v_hbm, tk_hbm, tv_hbm, img_hbm, gate_hbm, res_hbm, w_hbm,
    out_ref,
    img_ref, kv, qt, tk_ref, tv_ref, gate_ref, res_ref, qa, ka, va, acc, mx, tpad, s0, s1, osend, orecv, ssend, srecv, packed, arecv, wbuf,
    q_s, q_r, kv_s, kv_r, w_s, w_r, o_s, o_r, st_s, st_r, a_s, a_r, in_s, token,
):
    blk = lax.axis_index("blk")
    head = lax.axis_index("head")
    z = lax.div(blk, YL)
    y = lax.rem(blk, YL)
    zright = lax.rem(z + 1, ZL) * YL + y
    zleft = lax.rem(z + ZL - 1, ZL) * YL + y
    ypeer = [z * YL + flip(y, c, 2) for c in range(YL)]
    hpeer = [flip(head, s, 4) for s in range(NH)]

    barrier = pltpu.get_barrier_semaphore()
    for other in (zright, zleft, ypeer[1], ypeer[2], ypeer[3]):
        pl.semaphore_signal(barrier, inc=1, device_id={"blk": other}, device_id_type=MESH)
    for s in (4, 12, 8, 2, 1):
        pl.semaphore_signal(barrier, inc=1, device_id={"head": hpeer[s]}, device_id_type=MESH)

    loads = [
        pltpu.make_async_copy(src, dst, in_s.at[n])
        for n, (src, dst) in enumerate((
            (img_hbm, img_ref),
            (q_hbm, qt.at[0]),
            (k_hbm, kv.at[0, pl.ds(0, HD)]),
            (v_hbm, kv.at[0, pl.ds(HD, HD)]),
            (w_hbm, wbuf.at[pl.ds(0, HD)]),
            (tk_hbm, tk_ref),
            (tv_hbm, tv_ref),
            (gate_hbm, gate_ref),
            (res_hbm, res_ref),
        ))
    ]
    for cp in loads:
        cp.start()

    def send(src, dst, ssem, rsem, dev):
        copy = pltpu.make_async_remote_copy(
            src_ref=src, dst_ref=dst, send_sem=ssem, recv_sem=rsem,
            device_id=dev, device_id_type=MESH,
        )
        copy.start()
        return copy

    def settle(ref, sem, sent=False):
        copy = pltpu.make_async_remote_copy(
            src_ref=ref, dst_ref=ref, send_sem=sem, recv_sem=sem,
            device_id={"head": hpeer[1]}, device_id_type=MESH,
        )
        if sent:
            copy.wait_send()
        else:
            copy.wait_recv()

    def q_copy(c):
        return send(qt.at[0], qt.at[c], q_s, q_r.at[c - 1], {"blk": ypeer[c]})

    kv_cps = {}

    def kv_send(kind, step, half):
        src = step - 1 if kind in ("lk", "lv") or step == 1 else ZL - (step - 1)
        dst = step if kind in ("lk", "lv") else ZL - step
        k = 2 * ({"rk": 0, "rv": 4, "lk": 7, "lv": 10}[kind] + step - 1) + half
        rows = pl.ds((0 if kind in ("rk", "lk") else HD) + half * (HD // 2), HD // 2)
        dev = {"blk": zleft if kind in ("lk", "lv") else zright}
        kv_cps[kind, step, half] = send(kv.at[src, rows], kv.at[dst, rows], kv_s, kv_r.at[k], dev)

    def kv_hop(part, step):
        for half in range(2):
            for kind in ("r" + part, "l" + part):
                if (kind, step, half) in kv_cps:
                    kv_cps[kind, step, half].wait_recv()
                    if step < {"rk": 4, "lk": 3, "rv": 3, "lv": 4}[kind]:
                        kv_send(kind, step + 1, half)

    def w_part(slot, half):
        if half is None:
            return wbuf.at[pl.ds(slot * HD, HD)]
        return wbuf.at[pl.ds(slot * HD + half * (HD // WQ), HD // WQ)]

    def w_copy(origin, to, half=None):
        slot = origin ^ to
        if slot == 2:
            sem = w_r.at[half]
        elif slot % 2:
            sem = w_r.at[WQ]
        else:
            sem = w_r.at[WQ + 1 if slot in (4, 12, 8) else WQ + 2]
        send(w_part(origin, half), w_part(slot, half), w_s, sem, {"head": hpeer[to]})

    def fill_keys(slot, first_block):
        row = iota((HD, BS), 0)
        gaps = []
        for b in range(TOK // BS):
            image = img_ref[first_block + b]
            gaps.append(jnp.where((row < 8) & (row != image), FAR, 0.0))
        wide = jnp.concatenate([kv[slot, 0:HD].astype(F32), jnp.concatenate(gaps, axis=1)], axis=0)
        ka[slot] = wide.T.astype(BF)

    def fill_values(slot):
        va[slot, 0:HD] = kv[slot, HD : 2 * HD]
        va[slot, HD : HD + 16] = jnp.ones((16, TOK), BF)

    def fill_queries(c):
        qa[c, 0:HD] = qt[c]
        first = ypeer[c] * (TOK // BS)
        for b in range(TOK // BS):
            image = img_ref[first + b]
            hot = (iota((16, BS), 0) == image).astype(F32)
            qa[c, HD : HD + 16, b * BS : (b + 1) * BS] = hot.astype(BF)
        qa[c, HD + 16 : 128] = jnp.zeros((128 - HD - 16, TOK), BF)

    seen = set()
    pending = []
    turn = [0]

    def scores(slot, c, n, buf):
        sc = jnp.dot(ka[slot, 0:n], qa[c], preferred_element_type=F32)
        buf[0:n] = sc
        buf[TOK : TOK + 8] = jnp.max(sc.reshape(n // 8, 8, TOK), axis=0)

    def soften(slot, c, n, buf):
        new = jnp.max(buf[TOK : TOK + 8], axis=0, keepdims=True)
        if c in seen:
            old = mx[c, 0:1]
            new = jnp.maximum(old, new)
            shrink = jnp.exp2((old - new) * RATE)
        pr = jnp.exp2((buf[0:n] - new) * RATE).astype(BF)
        upd = jnp.dot(va[slot, :, 0:n], pr, preferred_element_type=F32)
        if c in seen:
            acc[c] = acc[c] * shrink + upd
        else:
            acc[c] = upd
        mx[c, 0:1] = new
        seen.add(c)

    def flush():
        while pending:
            soften(*pending.pop(0))

    def steps(*pairs):
        for slot, c in pairs:
            n = tail if slot == ZL + TSLOTS - 1 else TOK
            buf = (s0, s1)[turn[0] % 2]
            turn[0] += 1
            scores(slot, c, n, buf)
            flush()
            pending.append((slot, c, n, buf))

    def origin_block(slot):
        return (lax.rem(z + slot, ZL) * YL + y) * (TOK // BS)

    def send_part(c):
        osend[c - 1] = acc[c, 0:HD].astype(BF)
        for a in range(4):
            ssend[c - 1, a : a + 1] = mx[c, 0:1, a * 128 : (a + 1) * 128]
            ssend[c - 1, 4 + a : 5 + a] = acc[c, HD : HD + 1, a * 128 : (a + 1) * 128]
        dev = {"blk": ypeer[c]}
        send(osend.at[c - 1], orecv.at[c - 1], o_s, o_r, dev)
        send(ssend.at[c - 1], srecv.at[c - 1], st_s, st_r, dev)

    ntext = tk_hbm.shape[1]
    edge = (TSLOTS - 1) * TOK
    tail = -(-(ntext - edge) // 128) * 128
    for cp in loads[:4]:
        cp.wait()
    with jax.named_scope("barrier"):
        pl.semaphore_wait(barrier, 10)

    q_cps = [None] + [q_copy(c) for c in (1, 2, 3)]
    for part in ("k", "v"):
        for half in range(2):
            kv_send("r" + part, 1, half)
            kv_send("l" + part, 1, half)
    pl.semaphore_signal(token.at[0], inc=1, device_id={"head": hpeer[2]}, device_id_type=MESH)
    loads[4].wait()
    for s in (4, 12, 8):
        w_copy(0, s)
    w_copy(0, 1)

    fill_queries(0)
    fill_keys(0, blk * (TOK // BS))
    fill_values(0)
    loads[5].wait()
    loads[6].wait()
    for n, ref in ((0, tk_ref), (1, tv_ref)):
        tpad[n, :, edge:] = jnp.zeros((HD, TOK), BF)
        tpad[n, :, 0:ntext] = ref[...]
    for t in range(TSLOTS):
        row = iota((HD, TOK), 0)
        col = iota((HD, TOK), 1) + t * TOK
        inside = (col >= row * TEXT) & (col < (row + 1) * TEXT)
        gap = jnp.where((row < 8) & jnp.logical_not(inside), FAR, 0.0)
        span = slice(t * TOK, (t + 1) * TOK)
        wide = jnp.concatenate([tpad[0, :, span].astype(F32), gap], axis=0)
        ka[ZL + t] = wide.T.astype(BF)
        va[ZL + t, 0:HD] = tpad[1, :, span]
        va[ZL + t, HD : HD + 16] = jnp.ones((16, TOK), BF)

    with jax.named_scope("text"):
        steps((8, 0), (9, 0), (10, 0), (0, 0))
        flush()
    def w_hop(quarter):
        with jax.named_scope("wy%d" % quarter):
            settle(w_part(2, quarter), w_r.at[quarter])
        for s in (4, 12, 8):
            w_copy(2, s, quarter)

    with jax.named_scope("k1"):
        kv_hop("k", 1)
    fill_keys(7, origin_block(7))
    fill_keys(1, origin_block(1))
    steps((7, 0))
    with jax.named_scope("v1"):
        kv_hop("v", 1)
    fill_values(7)
    fill_values(1)
    steps((1, 0))
    with jax.named_scope("qwait1"):
        q_cps[1].wait_recv()
    w_copy(0, 2, 0)
    pl.semaphore_wait(token.at[0], 1)
    pl.semaphore_signal(token.at[1], inc=1, device_id={"head": hpeer[1]}, device_id_type=MESH)
    fill_queries(1)
    steps((0, 1), (7, 1), (1, 1))
    with jax.named_scope("k2"):
        kv_hop("k", 2)
    fill_keys(6, origin_block(6))
    fill_keys(2, origin_block(2))
    with jax.named_scope("qwait2"):
        q_cps[2].wait_recv()
    w_copy(0, 2, 1)
    fill_queries(2)
    steps((0, 2), (7, 2), (1, 2))
    with jax.named_scope("v2"):
        kv_hop("v", 2)
    w_copy(0, 2, 2)
    fill_values(6)
    fill_values(2)
    steps((6, 1), (2, 1), (6, 2), (2, 2))
    with jax.named_scope("k3"):
        kv_hop("k", 3)
    fill_keys(5, origin_block(5))
    fill_keys(3, origin_block(3))
    w_copy(0, 2, 3)
    with jax.named_scope("qwait3"):
        q_cps[3].wait_recv()
    fill_queries(3)
    steps((0, 3), (7, 3), (1, 3), (5, 1))
    with jax.named_scope("v3"):
        kv_hop("v", 3)
    fill_values(5)
    fill_values(3)
    steps((3, 1), (6, 3), (2, 3))
    with jax.named_scope("k4"):
        kv_hop("k", 4)
    fill_keys(4, origin_block(4))
    settle(wbuf.at[pl.ds(0, 3 * HD)], w_r.at[WQ + 1])
    for s in (4, 12, 8):
        w_copy(s, 1)
    w_hop(0)
    steps((5, 3), (3, 3), (5, 2), (3, 2), (4, 3))
    with jax.named_scope("v4"):
        kv_hop("v", 4)
    w_hop(1)
    fill_values(4)
    steps((4, 2))
    send_part(3)
    w_hop(2)
    steps((4, 1))
    send_part(2)
    steps((5, 0))
    send_part(1)
    w_hop(3)
    w_copy(2, 1)
    steps((3, 0), (4, 0), (6, 0), (2, 0))
    flush()
    pl.semaphore_wait(token.at[1], 1)
    with jax.named_scope("owait"):
        settle(orecv, o_r)
        settle(srecv, st_r)

    def row_of(ref, c, first):
        return jnp.concatenate([ref[c - 1, first + a : first + a + 1] for a in range(4)], axis=1)

    maxes = [mx[0, 0:1]] + [row_of(srecv, c, 0) for c in (1, 2, 3)]
    sums = [acc[0, HD : HD + 1]] + [row_of(srecv, c, 4) for c in (1, 2, 3)]
    top = functools.reduce(jnp.maximum, maxes)
    scales = [jnp.exp2((m - top) * RATE) for m in maxes]
    denom = functools.reduce(jnp.add, [s * l for s, l in zip(scales, sums)])
    numer = acc[0, 0:HD] * scales[0]
    for c in (1, 2, 3):
        numer = numer + orecv[c - 1].astype(F32) * scales[c]
    att = numer / denom
    both = jnp.concatenate([att, att], axis=0).T
    half = ROWS // 2
    side = iota((half, 128), 1) < HD
    for j in range(NH):
        one = both[j * ROWS : j * ROWS + half]
        two = both[j * ROWS + half : (j + 1) * ROWS]
        packed[j] = jnp.where(side, one, two).astype(BF)

    for s in (10, 11, 2, 3, 6, 7, 14, 15, 8, 9, 4, 5, 12, 13, 1):
        send(packed.at[hpeer[s]], arecv.at[s - 1], a_s, a_r, {"head": hpeer[s]})
    with jax.named_scope("wxwait2"):
        settle(wbuf.at[pl.ds(0, 3 * HD)], w_r.at[WQ + 2])
    for s in (6, 14, 10):
        w_copy(s, 1)
    mine = packed[head].astype(F32)
    with jax.named_scope("await"):
        settle(arecv, a_r)
    loads[7].wait()
    loads[8].wait()
    with jax.named_scope("wcwait"):
        settle(wbuf.at[pl.ds(0, NH // 2 * HD)], w_r.at[WQ])
    pairs = []
    for i in range(NH // 2):
        even = mine if i == 0 else arecv[2 * i - 1].astype(F32)
        odd = arecv[2 * i].astype(F32)
        upper = jnp.where(side, even, pltpu.roll(odd, HD, 1))
        lower = jnp.where(side, pltpu.roll(even, HD, 1), odd)
        pairs.append(jnp.concatenate([upper, lower], axis=0).astype(BF))
    mixed = jnp.concatenate(pairs, axis=1)
    image = img_ref[blk * (TOK // BS) + lax.div(head, NH * BS // TOK)]
    gating = gate_ref[pl.ds(image, 1), :]
    projected = jnp.dot(mixed, wbuf[...], preferred_element_type=F32)
    out_ref[...] = (res_ref[...].astype(F32) + gating * projected).astype(BF)
    with jax.named_scope("sendwait"):
        settle(qt.at[pl.ds(1, 3)], q_s, True)
        settle(kv.at[pl.ds(0, 7)], kv_s, True)
        settle(wbuf.at[pl.ds(0, 15 * HD)], w_s, True)
        settle(osend, o_s, True)
        settle(ssend, st_s, True)
        settle(arecv, a_s, True)


def on_device(queries, key_rows, values, text_keys, text_values, block_image, gate_image, residual, w_out):
    vm = pl.BlockSpec(memory_space=pltpu.VMEM)
    hb = pl.BlockSpec(memory_space=pl.ANY)
    dma = pltpu.SemaphoreType.DMA
    return pl.pallas_call(
        kernel,
        out_shape=pltpu.VMEM((ROWS, D), BF),
        in_specs=[hb] * 9,
        out_specs=vm,
        scratch_shapes=[
            pltpu.SMEM(block_image.shape, jnp.int32),
            pltpu.VMEM((ZL, 2 * HD, TOK), BF),
            pltpu.VMEM((YL, HD, TOK), BF),
            pltpu.VMEM((HD, text_keys.shape[0]), BF),
            pltpu.VMEM((HD, text_keys.shape[0]), BF),
            pltpu.VMEM(gate_image.shape, F32),
            pltpu.VMEM((ROWS, D), BF),
            pltpu.VMEM((YL, 128, TOK), BF),
            pltpu.VMEM((ZL + TSLOTS, TOK, 128), BF),
            pltpu.VMEM((ZL + TSLOTS, HD + 16, TOK), BF),
            pltpu.VMEM((YL, HD + 16, TOK), F32),
            pltpu.VMEM((YL, 8, TOK), F32),
            pltpu.VMEM((2, HD, TSLOTS * TOK), BF),
            pltpu.VMEM((TOK + 8, TOK), F32),
            pltpu.VMEM((TOK + 8, TOK), F32),
            pltpu.VMEM((3, HD, TOK), BF),
            pltpu.VMEM((3, HD, TOK), BF),
            pltpu.VMEM((3, 8, 128), F32),
            pltpu.VMEM((3, 8, 128), F32),
            pltpu.VMEM((NH, ROWS // 2, 128), BF),
            pltpu.VMEM((NH - 1, ROWS // 2, 128), BF),
            pltpu.VMEM((NH * HD, D), BF),
            dma, dma((3,)),
            dma, dma((28,)),
            dma, dma((WQ + 3,)),
            dma, dma,
            dma, dma,
            dma, dma,
            dma((9,)),
            pltpu.SemaphoreType.REGULAR((2,)),
        ],
        compiler_params=pltpu.CompilerParams(
            collective_id=0, has_side_effects=True, vmem_limit_bytes=60 * 1024 * 1024
        ),
        name="joint_attention",
    )(
        queries.T, key_rows.T, values.T, text_keys.T, text_values.T,
        block_image, gate_image, residual, w_out,
    )


def solution(mesh):
    placed = (
        P("blk", "head"),
        P("blk", "head"),
        P("blk", "head"),
        P(None, "head"),
        P(None, "head"),
        P(),
        P(),
        P(("blk", "head"), None),
        P("head", None),
    )
    return jax.shard_map(
        on_device, mesh=mesh, in_specs=placed, out_specs=P(("blk", "head"), None), check_vma=False
    )
```

```python
import functools
import math

import jax
import jax.numpy as jnp
from jax import lax
from jax.experimental import pallas as pl
from jax.experimental.pallas import tpu as pltpu
from jax.sharding import PartitionSpec as P

HD = 64
TEXT = 154
BS = 128
TOK = 512
YL = 4
ZL = 8
NH = 16
D = 1536
ROWS = TOK // NH
TSLOTS = 3
WQ = 4
FAR = -(2.0**100)
RATE = math.log2(math.e) / math.sqrt(HD)
MESH = pl.DeviceIdType.MESH
BF = jnp.bfloat16
F32 = jnp.float32
NT = (((1,), (1,)), ((), ()))


def flip(index, mask, bits):
    total = 0
    for b in range(bits):
        bit = lax.rem(lax.div(index, 1 << b), 2)
        total = total + (1 << b) * ((1 - bit) if (mask >> b) & 1 else bit)
    return total


def iota(shape, dim):
    return lax.broadcasted_iota(jnp.int32, shape, dim)


def kernel(
    q_hbm, k_hbm, v_hbm, tk_hbm, tv_hbm, img_hbm, gate_hbm, res_hbm, w_hbm,
    out_ref,
    img_ref, kv, qt, tk_ref, tv_ref, gate_ref, res_ref, qa, ka, va, acc, mx, tpad, s0, s1, osend, orecv, ssend, srecv, packed, arecv, wbuf,
    q_s, q_r, kv_s, kv_r, w_s, w_r, o_s, o_r, st_s, st_r, a_s, a_r, in_s, token,
):
    blk = lax.axis_index("blk")
    head = lax.axis_index("head")
    z = lax.div(blk, YL)
    y = lax.rem(blk, YL)
    zright = lax.rem(z + 1, ZL) * YL + y
    zleft = lax.rem(z + ZL - 1, ZL) * YL + y
    ypeer = [z * YL + flip(y, c, 2) for c in range(YL)]
    hpeer = [flip(head, s, 4) for s in range(NH)]

    barrier = pltpu.get_barrier_semaphore()
    for other in (zright, zleft, ypeer[1], ypeer[2], ypeer[3]):
        pl.semaphore_signal(barrier, inc=1, device_id={"blk": other}, device_id_type=MESH)
    for s in (4, 12, 8, 2, 1):
        pl.semaphore_signal(barrier, inc=1, device_id={"head": hpeer[s]}, device_id_type=MESH)

    loads = [
        pltpu.make_async_copy(src, dst, in_s.at[2 if n == 3 else n])
        for n, (src, dst) in enumerate((
            (img_hbm, img_ref),
            (q_hbm, qt.at[0]),
            (k_hbm, kv.at[0, pl.ds(0, HD)]),
            (v_hbm, kv.at[0, pl.ds(HD, HD)]),
            (w_hbm, wbuf.at[pl.ds(0, HD)]),
            (tk_hbm, tk_ref),
            (tv_hbm, tv_ref),
            (gate_hbm, gate_ref),
            (res_hbm, res_ref),
        ))
    ]
    for cp in loads:
        cp.start()

    def send(src, dst, ssem, rsem, dev):
        copy = pltpu.make_async_remote_copy(
            src_ref=src, dst_ref=dst, send_sem=ssem, recv_sem=rsem,
            device_id=dev, device_id_type=MESH,
        )
        copy.start()
        return copy

    def settle(ref, sem, sent=False):
        copy = pltpu.make_async_remote_copy(
            src_ref=ref, dst_ref=ref, send_sem=sem, recv_sem=sem,
            device_id={"head": hpeer[1]}, device_id_type=MESH,
        )
        if sent:
            copy.wait_send()
        else:
            copy.wait_recv()

    def q_copy(c):
        return send(qt.at[0], qt.at[c], q_s, q_r.at[c - 1], {"blk": ypeer[c]})

    kv_cps = {}

    def kv_send(kind, step, half):
        src = step - 1 if kind in ("lk", "lv") or step == 1 else ZL - (step - 1)
        dst = step if kind in ("lk", "lv") else ZL - step
        k = 2 * ({"rk": 0, "rv": 4, "lk": 7, "lv": 10}[kind] + step - 1) + half
        rows = pl.ds((0 if kind in ("rk", "lk") else HD) + half * (HD // 2), HD // 2)
        dev = {"blk": zleft if kind in ("lk", "lv") else zright}
        kv_cps[kind, step, half] = send(kv.at[src, rows], kv.at[dst, rows], kv_s, kv_r.at[k], dev)

    def kv_hop(part, step):
        for half in range(2):
            for kind in ("r" + part, "l" + part):
                if (kind, step, half) in kv_cps:
                    kv_cps[kind, step, half].wait_recv()
                    if step < {"rk": 4, "lk": 3, "rv": 3, "lv": 4}[kind]:
                        kv_send(kind, step + 1, half)

    def w_part(slot, half):
        if half is None:
            return wbuf.at[pl.ds(slot * HD, HD)]
        return wbuf.at[pl.ds(slot * HD + half * (HD // WQ), HD // WQ)]

    def w_copy(origin, to, half=None):
        slot = origin ^ to
        if slot == 2:
            sem = w_r.at[half]
        elif slot % 2:
            sem = w_r.at[WQ]
        else:
            sem = w_r.at[WQ + 1 if slot in (4, 12, 8) else WQ + 2]
        send(w_part(origin, half), w_part(slot, half), w_s, sem, {"head": hpeer[to]})

    def fill_keys(slot, first_block):
        row = iota((HD, BS), 0)
        gaps = []
        for b in range(TOK // BS):
            image = img_ref[first_block + b]
            gaps.append(jnp.where((row < 8) & (row != image), FAR, 0.0))
        wide = jnp.concatenate([kv[slot, 0:HD].astype(F32), jnp.concatenate(gaps, axis=1)], axis=0)
        ka[slot] = wide.T.astype(BF)
        va[slot, 0:HD] = kv[slot, HD : 2 * HD]
        va[slot, HD : HD + 16] = jnp.ones((16, TOK), BF)

    def fill_queries(c):
        qa[c, 0:HD] = qt[c]
        first = ypeer[c] * (TOK // BS)
        for b in range(TOK // BS):
            image = img_ref[first + b]
            hot = (iota((16, BS), 0) == image).astype(F32)
            qa[c, HD : HD + 16, b * BS : (b + 1) * BS] = hot.astype(BF)
        qa[c, HD + 16 : 128] = jnp.zeros((128 - HD - 16, TOK), BF)

    seen = set()
    pending = []
    turn = [0]

    def scores(slot, c, n, buf):
        sc = jnp.dot(ka[slot, 0:n], qa[c], preferred_element_type=F32)
        buf[0:n] = sc
        buf[TOK : TOK + 8] = jnp.max(sc.reshape(n // 8, 8, TOK), axis=0)

    def soften(slot, c, n, buf):
        new = jnp.max(buf[TOK : TOK + 8], axis=0, keepdims=True)
        if c in seen:
            old = mx[c, 0:1]
            new = jnp.maximum(old, new)
            shrink = jnp.exp2((old - new) * RATE)
        pr = jnp.exp2((buf[0:n] - new) * RATE).astype(BF)
        upd = jnp.dot(va[slot, :, 0:n], pr, preferred_element_type=F32)
        if c in seen:
            acc[c] = acc[c] * shrink + upd
        else:
            acc[c] = upd
        mx[c, 0:1] = new
        seen.add(c)

    def flush():
        while pending:
            soften(*pending.pop(0))

    def steps(*pairs):
        for slot, c in pairs:
            n = tail if slot == ZL + TSLOTS - 1 else TOK
            buf = (s0, s1)[turn[0] % 2]
            turn[0] += 1
            scores(slot, c, n, buf)
            flush()
            pending.append((slot, c, n, buf))

    def origin_block(slot):
        return (lax.rem(z + slot, ZL) * YL + y) * (TOK // BS)

    def send_part(c):
        osend[c - 1] = acc[c, 0:HD].astype(BF)
        for a in range(4):
            ssend[c - 1, a : a + 1] = mx[c, 0:1, a * 128 : (a + 1) * 128]
            ssend[c - 1, 4 + a : 5 + a] = acc[c, HD : HD + 1, a * 128 : (a + 1) * 128]
        dev = {"blk": ypeer[c]}
        send(osend.at[c - 1], orecv.at[c - 1], o_s, o_r, dev)
        send(ssend.at[c - 1], srecv.at[c - 1], st_s, st_r, dev)

    ntext = tk_hbm.shape[1]
    edge = (TSLOTS - 1) * TOK
    tail = -(-(ntext - edge) // 128) * 128
    for cp in loads[:2]:
        cp.wait()
    pltpu.make_async_copy(kv.at[0], kv.at[0], in_s.at[2]).wait()
    with jax.named_scope("barrier"):
        pl.semaphore_wait(barrier, 10)

    q_cps = [None] + [q_copy(c) for c in (1, 2, 3)]
    for part in ("k", "v"):
        for half in range(2):
            kv_send("r" + part, 1, half)
            kv_send("l" + part, 1, half)
    pl.semaphore_signal(token.at[0], inc=1, device_id={"head": hpeer[2]}, device_id_type=MESH)
    loads[4].wait()
    for s in (4, 12, 8):
        w_copy(0, s)
    w_copy(0, 1)

    fill_queries(0)
    fill_keys(0, blk * (TOK // BS))
    loads[5].wait()
    loads[6].wait()
    for n, ref in ((0, tk_ref), (1, tv_ref)):
        tpad[n, :, edge:] = jnp.zeros((HD, TOK), BF)
        tpad[n, :, 0:ntext] = ref[...]
    for t in range(TSLOTS):
        row = iota((HD, TOK), 0)
        col = iota((HD, TOK), 1) + t * TOK
        inside = (col >= row * TEXT) & (col < (row + 1) * TEXT)
        gap = jnp.where((row < 8) & jnp.logical_not(inside), FAR, 0.0)
        span = slice(t * TOK, (t + 1) * TOK)
        wide = jnp.concatenate([tpad[0, :, span].astype(F32), gap], axis=0)
        ka[ZL + t] = wide.T.astype(BF)
        va[ZL + t, 0:HD] = tpad[1, :, span]
        va[ZL + t, HD : HD + 16] = jnp.ones((16, TOK), BF)

    with jax.named_scope("text"):
        steps((8, 0), (9, 0), (10, 0), (0, 0))
        flush()
    with jax.named_scope("k1"):
        kv_hop("k", 1)
    with jax.named_scope("v1"):
        kv_hop("v", 1)
    fill_keys(7, origin_block(7))
    fill_keys(1, origin_block(1))
    steps((7, 0), (1, 0))
    with jax.named_scope("qwait1"):
        q_cps[1].wait_recv()
    w_copy(0, 2, 0)
    pl.semaphore_wait(token.at[0], 1)
    pl.semaphore_signal(token.at[1], inc=1, device_id={"head": hpeer[1]}, device_id_type=MESH)
    fill_queries(1)
    steps((0, 1), (7, 1), (1, 1))
    with jax.named_scope("k2"):
        kv_hop("k", 2)
    with jax.named_scope("qwait2"):
        q_cps[2].wait_recv()
    w_copy(0, 2, 1)
    fill_queries(2)
    steps((0, 2), (7, 2), (1, 2))
    with jax.named_scope("v2"):
        kv_hop("v", 2)
    w_copy(0, 2, 2)
    fill_keys(6, origin_block(6))
    fill_keys(2, origin_block(2))
    steps((6, 1), (2, 1), (6, 2), (2, 2))
    with jax.named_scope("k3"):
        kv_hop("k", 3)
    w_copy(0, 2, 3)
    with jax.named_scope("qwait3"):
        q_cps[3].wait_recv()
    fill_queries(3)
    steps((0, 3), (7, 3))
    steps((1, 3))
    with jax.named_scope("v3"):
        kv_hop("v", 3)
    fill_keys(5, origin_block(5))
    fill_keys(3, origin_block(3))
    steps((5, 1), (3, 1), (6, 3), (2, 3))
    def w_hop(quarter):
        with jax.named_scope("wy%d" % quarter):
            settle(w_part(2, quarter), w_r.at[quarter])
        for s in (4, 12, 8):
            w_copy(2, s, quarter)

    with jax.named_scope("k4"):
        kv_hop("k", 4)
    settle(wbuf.at[pl.ds(0, 3 * HD)], w_r.at[WQ + 1])
    for s in (4, 12, 8):
        w_copy(s, 1)
    w_hop(0)
    steps((5, 3), (3, 3))
    with jax.named_scope("v4"):
        kv_hop("v", 4)
    w_hop(1)
    fill_keys(4, origin_block(4))
    steps((4, 3), (5, 2))
    send_part(3)
    w_hop(2)
    steps((3, 2), (4, 2), (4, 1))
    send_part(2)
    w_hop(3)
    w_copy(2, 1)
    steps((5, 0))
    send_part(1)
    steps((3, 0), (4, 0), (6, 0), (2, 0))
    flush()
    pl.semaphore_wait(token.at[1], 1)
    with jax.named_scope("owait"):
        settle(orecv, o_r)
        settle(srecv, st_r)

    def row_of(ref, c, first):
        return jnp.concatenate([ref[c - 1, first + a : first + a + 1] for a in range(4)], axis=1)

    maxes = [mx[0, 0:1]] + [row_of(srecv, c, 0) for c in (1, 2, 3)]
    sums = [acc[0, HD : HD + 1]] + [row_of(srecv, c, 4) for c in (1, 2, 3)]
    top = functools.reduce(jnp.maximum, maxes)
    scales = [jnp.exp2((m - top) * RATE) for m in maxes]
    denom = functools.reduce(jnp.add, [s * l for s, l in zip(scales, sums)])
    numer = acc[0, 0:HD] * scales[0]
    for c in (1, 2, 3):
        numer = numer + orecv[c - 1].astype(F32) * scales[c]
    att = numer / denom
    both = jnp.concatenate([att, att], axis=0).T
    half = ROWS // 2
    side = iota((half, 128), 1) < HD
    for j in range(NH):
        one = both[j * ROWS : j * ROWS + half]
        two = both[j * ROWS + half : (j + 1) * ROWS]
        packed[j] = jnp.where(side, one, two).astype(BF)

    for s in (10, 11, 2, 3, 6, 7, 14, 15, 8, 9, 4, 5, 12, 13, 1):
        send(packed.at[hpeer[s]], arecv.at[s - 1], a_s, a_r, {"head": hpeer[s]})
    with jax.named_scope("wxwait2"):
        settle(wbuf.at[pl.ds(0, 3 * HD)], w_r.at[WQ + 2])
    for s in (6, 14, 10):
        w_copy(s, 1)
    mine = packed[head].astype(F32)
    with jax.named_scope("await"):
        settle(arecv, a_r)
    loads[7].wait()
    loads[8].wait()
    with jax.named_scope("wcwait"):
        settle(wbuf.at[pl.ds(0, NH // 2 * HD)], w_r.at[WQ])
    pairs = []
    for i in range(NH // 2):
        even = mine if i == 0 else arecv[2 * i - 1].astype(F32)
        odd = arecv[2 * i].astype(F32)
        upper = jnp.where(side, even, pltpu.roll(odd, HD, 1))
        lower = jnp.where(side, pltpu.roll(even, HD, 1), odd)
        pairs.append(jnp.concatenate([upper, lower], axis=0).astype(BF))
    mixed = jnp.concatenate(pairs, axis=1)
    image = img_ref[blk * (TOK // BS) + lax.div(head, NH * BS // TOK)]
    gating = gate_ref[pl.ds(image, 1), :]
    projected = jnp.dot(mixed, wbuf[...], preferred_element_type=F32)
    out_ref[...] = (res_ref[...].astype(F32) + gating * projected).astype(BF)
    with jax.named_scope("sendwait"):
        settle(qt.at[pl.ds(1, 3)], q_s, True)
        settle(kv.at[pl.ds(0, 7)], kv_s, True)
        settle(wbuf.at[pl.ds(0, 15 * HD)], w_s, True)
        settle(osend, o_s, True)
        settle(ssend, st_s, True)
        settle(arecv, a_s, True)


def on_device(queries, key_rows, values, text_keys, text_values, block_image, gate_image, residual, w_out):
    vm = pl.BlockSpec(memory_space=pltpu.VMEM)
    hb = pl.BlockSpec(memory_space=pl.ANY)
    dma = pltpu.SemaphoreType.DMA
    return pl.pallas_call(
        kernel,
        out_shape=pltpu.VMEM((ROWS, D), BF),
        in_specs=[hb] * 9,
        out_specs=vm,
        scratch_shapes=[
            pltpu.SMEM(block_image.shape, jnp.int32),
            pltpu.VMEM((ZL, 2 * HD, TOK), BF),
            pltpu.VMEM((YL, HD, TOK), BF),
            pltpu.VMEM((HD, text_keys.shape[0]), BF),
            pltpu.VMEM((HD, text_keys.shape[0]), BF),
            pltpu.VMEM(gate_image.shape, F32),
            pltpu.VMEM((ROWS, D), BF),
            pltpu.VMEM((YL, 128, TOK), BF),
            pltpu.VMEM((ZL + TSLOTS, TOK, 128), BF),
            pltpu.VMEM((ZL + TSLOTS, HD + 16, TOK), BF),
            pltpu.VMEM((YL, HD + 16, TOK), F32),
            pltpu.VMEM((YL, 8, TOK), F32),
            pltpu.VMEM((2, HD, TSLOTS * TOK), BF),
            pltpu.VMEM((TOK + 8, TOK), F32),
            pltpu.VMEM((TOK + 8, TOK), F32),
            pltpu.VMEM((3, HD, TOK), BF),
            pltpu.VMEM((3, HD, TOK), BF),
            pltpu.VMEM((3, 8, 128), F32),
            pltpu.VMEM((3, 8, 128), F32),
            pltpu.VMEM((NH, ROWS // 2, 128), BF),
            pltpu.VMEM((NH - 1, ROWS // 2, 128), BF),
            pltpu.VMEM((NH * HD, D), BF),
            dma, dma((3,)),
            dma, dma((28,)),
            dma, dma((WQ + 3,)),
            dma, dma,
            dma, dma,
            dma, dma,
            dma((9,)),
            pltpu.SemaphoreType.REGULAR((2,)),
        ],
        compiler_params=pltpu.CompilerParams(
            collective_id=0, has_side_effects=True, vmem_limit_bytes=60 * 1024 * 1024
        ),
        name="joint_attention",
    )(
        queries.T, key_rows.T, values.T, text_keys.T, text_values.T,
        block_image, gate_image, residual, w_out,
    )


def solution(mesh):
    placed = (
        P("blk", "head"),
        P("blk", "head"),
        P("blk", "head"),
        P(None, "head"),
        P(None, "head"),
        P(),
        P(),
        P(("blk", "head"), None),
        P("head", None),
    )
    return jax.shard_map(
        on_device, mesh=mesh, in_specs=placed, out_specs=P(("blk", "head"), None), check_vma=False
    )
```
